128 devices in a mesh: tile: 64 (over x, z, y), lev: 2 (over core).
Axes of the slice: x: 4, y: 4, z: 4, core: 2. Of those that a mesh axis runs over, the one named last changes fastest.
Arguments:
- increments: bfloat16 [136, 1024, 1024], P('lev', 'tile'), may hold values from -30 to 30
- projection: bfloat16 [80, 136], replicated, may hold values from -0.5 to 0.5
- helmholtz: float32 [80], P('lev'), may hold values from 0.05 to 4
Outputs:
- solution: float32 [80, 1024, 1024], P('lev', 'tile')
- residual: float32 [80, 1024, 1024], P('lev', 'tile')
The draws below stay inside these ranges and needn't reach their ends.
All inputs are finite; a program needn't handle non-finite values.
Results may differ from the reference program's by a relative error of at most 0.00075.
Values may be sent and summed in bfloat16 or wider, within the bound.
A program may use at most 192 MiB of HBM per device.

```python
import math
import jax
import jax.numpy as jnp
import numpy as np
from jax import lax

LEVELS = 136
MODES = 80
S = 4
BLOCKS = 2
NY = 1024
NX = 1024


def lowpass(field):
    for repeat in range(2):
        field = 0.25 * (jnp.roll(field, 1, 1) + 2.0 * field + jnp.roll(field, -1, 1))
        field = 0.25 * (jnp.roll(field, 1, 2) + 2.0 * field + jnp.roll(field, -1, 2))
    return field


def draw_increments(key, part):
    key_base = jax.random.fold_in(key, 11)
    key_one, key_two = jax.random.split(key_base, 2)
    row_frac = (jnp.arange(NX, dtype=jnp.float32) / NX)[None, :, None]
    base = jnp.clip(jax.random.normal(key_one, (LEVELS, NX, NY), jnp.float32), -6.0, 6.0)
    smooth = lowpass(jnp.clip(jax.random.normal(key_two, (LEVELS, NX, NY), jnp.float32), -6.0, 6.0))
    values = base + 10.0 * row_frac * smooth
    return jnp.clip(values, -30.0, 30.0).astype(jnp.bfloat16)


def levels(stream_key, dims, cuts, least, high):
    loudness, own = 1.0, jax.random.fold_in(stream_key, 6)
    for axis_at, blocks in cuts:
        steps = jnp.exp(jax.random.uniform(jax.random.fold_in(own, axis_at), (blocks,), jnp.float32, least / len(cuts), high / len(cuts)))
        loudness = loudness * jnp.repeat(steps, dims[axis_at] // blocks).reshape([-1 if axis == axis_at else 1 for axis in range(len(dims))])
    return loudness


def normal_values(key, extent, deviation, bound, held_as=jnp.bfloat16):
    entries = deviation * jax.random.normal(key, extent, jnp.float32)
    return jnp.clip(entries, min=-bound, max=bound).astype(held_as)


def setup_inputs(seed: int = 0) -> dict:
    streams_of = jax.random.split(jax.random.key(seed), 4)
    increments = draw_increments(jax.random.fold_in(streams_of[3], 71), 0)
    projection = normal_values(streams_of[1], (MODES, LEVELS), LEVELS ** -0.5, 0.5)
    helmholtz = jnp.clip(jnp.exp(math.log(4.0) - 4.3820266 * jax.random.uniform(streams_of[2], (MODES,), jnp.float32) ** levels(streams_of[2], (MODES,), ((0, 2),), -0.2, 0.2)), 0.05, 4.0)
    return dict(increments=increments, projection=projection, helmholtz=helmholtz)


highest = lax.Precision.HIGHEST


def stencil(field, weight):
    padded = jnp.pad(field, 1)
    beside_all = padded[2:, 1:-1] + padded[:-2, 1:-1] + padded[1:-1, 2:] + padded[1:-1, :-2]
    return weight * beside_all


def shift_matrix():
    width = 2 * S + 1
    table = np.zeros((width, width), np.float32)
    for index in range(S):
        table[index + 1, index] = 1.0
    for index in range(S - 1):
        table[S + 2 + index, S + 1 + index] = 1.0
    return jnp.asarray(table, jnp.float32)


def quadratic(gram, left, right):
    return jnp.dot(left, jnp.dot(gram, right, precision=highest), precision=highest)


def solve_mode(inputs):
    rhs, weight = inputs
    width = 2 * S + 1
    shifter = shift_matrix()
    solution = jnp.zeros_like(rhs)
    resid = rhs
    direction = rhs
    for block_index in range(BLOCKS):
        vectors = [direction]
        current = direction
        for power_index in range(S):
            current = stencil(current, weight)
            vectors.append(current)
        vectors.append(resid)
        current = resid
        for power_index in range(S - 1):
            current = stencil(current, weight)
            vectors.append(current)
        basis = jnp.stack(vectors).reshape(width, -1)
        gram = jnp.dot(basis, basis.T, precision=highest)
        p_coef = jnp.zeros((width,), jnp.float32).at[0].set(1.0)
        r_coef = jnp.zeros((width,), jnp.float32).at[S + 1].set(1.0)
        x_coef = jnp.zeros((width,), jnp.float32)
        squares = quadratic(gram, r_coef, r_coef)
        for step_index in range(S):
            moved = p_coef - jnp.dot(shifter, p_coef, precision=highest)
            alpha = squares / quadratic(gram, p_coef, moved)
            x_coef = x_coef + alpha * p_coef
            r_coef = r_coef - alpha * moved
            fresh = quadratic(gram, r_coef, r_coef)
            p_coef = r_coef + (fresh / squares) * p_coef
            squares = fresh
        solution = solution + jnp.dot(x_coef, basis, precision=highest).reshape(rhs.shape)
        resid = jnp.dot(r_coef, basis, precision=highest).reshape(rhs.shape)
        direction = jnp.dot(p_coef, basis, precision=highest).reshape(rhs.shape)
    return solution, resid


def reference(increments, projection, helmholtz):
    flat = increments.reshape(LEVELS, NX * NY)
    modal = jnp.dot(projection, flat, preferred_element_type=jnp.float32).reshape(MODES, NX, NY)
    weights = 1.0 / (4.0 + helmholtz)
    solution, resid = lax.map(solve_mode, (modal, weights))
    return solution, resid
```

```python
import functools

import jax
import jax.numpy as jnp
from jax import lax
from jax.experimental import pallas as pl
from jax.experimental.pallas import tpu as pltpu
from jax.sharding import PartitionSpec as P

STEPS = 8
ROWS = 16
HALO = 8
EXT = ROWS + 2 * HALO
NEAR = 4
LANES = 128
FLAT = 216
MESH = pl.DeviceIdType.MESH


def flat(level, row):
    return 32 * level - level * level + row


def kernel(dims, inc_hbm, proj_ref, helm_ref, sol_hbm, res_hbm,
           fields, inc_own, inc_far, kron, grams, far_out, far_in, coef, gather,
           lev_send, lev_recv, load_sem, near_send, near_recv, far_send, far_recv,
           red_send, red_recv, out_sem):
    tile = lax.axis_index("tile")
    lev = lax.axis_index("lev")
    tiles = lax.axis_size("tile")
    levels, _, cells = inc_own.shape
    modes = fields.shape[1]
    groups = modes // 8
    chunk = cells // 4
    cols = cells // LANES
    other = 1 - lev
    has = (tile > 0, tile < tiles - 1)
    partner = (tile - 1, tile + 1)
    f32 = jnp.float32

    loads = []
    for c in range(4):
        part = pl.ds(c * chunk, chunk)
        load = pltpu.make_async_copy(inc_hbm.at[:, :, part], inc_own.at[:, :, part], load_sem.at[c])
        load.start()
        loads.append(load)

    barrier = pltpu.get_barrier_semaphore()
    pl.semaphore_signal(barrier, inc=1, device_id={"lev": other}, device_id_type=MESH)
    for side in range(2):
        there = lax.rem(tile + (tiles - 1 if side == 0 else 1), tiles)
        pl.semaphore_signal(barrier, inc=1, device_id={"tile": there}, device_id_type=MESH)
    places = []
    for stride, size in dims:
        place = lax.rem(lax.div(tile, stride), size)
        places.append(place)
        for step in range(1, size):
            there = tile + (lax.rem(place + step, size) - place) * stride
            pl.semaphore_signal(barrier, inc=1, device_id={"tile": there}, device_id_type=MESH)
    pl.semaphore_wait(barrier, 3 + sum(size - 1 for _, size in dims))

    sends = []
    for c in range(4):
        part = pl.ds(c * chunk, chunk)
        send = pltpu.make_async_remote_copy(
            src_ref=inc_hbm.at[:, :, part], dst_ref=inc_far.at[:, :, part],
            send_sem=lev_send.at[c], recv_sem=lev_recv.at[c],
            device_id={"lev": other}, device_id_type=MESH)
        send.start()
        sends.append(send)

    wide = levels * ROWS
    table = proj_ref[...].astype(f32)
    table = jnp.where(lev == 0, table[:modes], table[modes:])
    left, right = table[:, :levels], table[:, levels:]
    own_part = jnp.where(lev == 0, left, right)
    far_part = jnp.where(lev == 0, right, left)
    spread = (lax.broadcasted_iota(jnp.int32, (levels, wide), 1) // ROWS
              == lax.broadcasted_iota(jnp.int32, (levels, wide), 0))
    spread = jnp.where(spread, 1.0, 0.0).astype(jnp.bfloat16)
    at_row = lax.broadcasted_iota(jnp.int32, (modes, wide), 1) % ROWS
    for half, part in enumerate((own_part, far_part)):
        repeated = jnp.dot(part.astype(jnp.bfloat16), spread, preferred_element_type=f32)
        for pair in range(ROWS // 2):
            both = jnp.concatenate([
                jnp.where(at_row == 2 * pair, repeated, 0.0),
                jnp.where(at_row == 2 * pair + 1, repeated, 0.0)], axis=0)
            kron[half, pl.ds(2 * modes * pair, 2 * modes), :] = both.astype(jnp.bfloat16)

    lane8 = lax.broadcasted_iota(jnp.int32, (8, LANES), 1)
    sub8 = lax.broadcasted_iota(jnp.int32, (8, LANES), 0)
    shifts = jnp.zeros((8, LANES), f32)
    for mode in range(modes):
        shifts = jnp.where((lane8 == mode // 8) & (sub8 == mode % 8), helm_ref[mode], shifts)
    scale = 4.0 / (4.0 + shifts)

    for side, base in ((0, 0), (1, EXT - HALO)):
        @pl.when(jnp.logical_not(has[side]))
        def _():
            def clear(row, carry):
                fields[row + base] = jnp.zeros((modes, cells), f32)
                return carry
            lax.fori_loop(0, HALO, clear, 0)
    grams[...] = jnp.zeros_like(grams)

    for c in range(4):
        loads[c].wait()
        part = pl.ds(c * chunk, chunk)
        first = jnp.dot(kron[0], inc_own[:, :, part].reshape(wide, chunk), preferred_element_type=f32)
        fields[pl.ds(HALO, ROWS), :, part] = first.reshape(ROWS, modes, chunk)

    def near_copy(side, d, piece):
        mine = HALO + d - 1 if side == 0 else EXT - HALO - d
        theirs = EXT - HALO - 1 + d if side == 0 else HALO - d
        part = pl.ds(0, chunk) if piece == 0 else pl.ds(chunk, cells - chunk)
        return pltpu.make_async_remote_copy(
            src_ref=fields.at[mine, :, part], dst_ref=fields.at[theirs, :, part],
            send_sem=near_send.at[side, d - 1, piece], recv_sem=near_recv.at[1 - side, d - 1, piece],
            device_id={"tile": partner[side]}, device_id_type=MESH)

    def far_copy(side, d):
        return pltpu.make_async_remote_copy(
            src_ref=far_out.at[side, d - NEAR - 1], dst_ref=far_in.at[1 - side, d - NEAR - 1],
            send_sem=far_send.at[side, d - NEAR - 1], recv_sem=far_recv.at[1 - side, d - NEAR - 1],
            device_id={"tile": partner[side]}, device_id_type=MESH)

    for c in range(4):
        sends[c].wait_recv()
        part = pl.ds(c * chunk, chunk)
        second = jnp.dot(kron[1], inc_far[:, :, part].reshape(wide, chunk), preferred_element_type=f32)
        fields[pl.ds(HALO, ROWS), :, part] += second.reshape(ROWS, modes, chunk)
        if c in (0, 3):
            for d in range(1, NEAR + 1):
                for side in range(2):
                    @pl.when(has[side])
                    def _():
                        near_copy(side, d, 0 if c == 0 else 1).start()
    half = cells // 2
    for d in range(NEAR + 1, HALO + 1):
        for side in range(2):
            mine = HALO + d - 1 if side == 0 else EXT - HALO - d
            for group in range(groups):
                rows = pl.ds(8 * group, 8)
                both = jnp.concatenate(
                    [fields[mine, rows, pl.ds(0, half)], fields[mine, rows, pl.ds(half, half)]], axis=0)
                far_out[side, d - NEAR - 1, group] = both.astype(jnp.bfloat16)

            @pl.when(has[side])
            def _():
                far_copy(side, d).start()

    lane = lax.broadcasted_iota(jnp.int32, (modes, LANES), 1)
    at_first, at_last = lane == 0, lane == LANES - 1

    def row_step(level, row, start, gram, keep=None):
        here = flat(level - 1, row)
        old = None if start else flat(level - 2, row)
        new = flat(level, row)
        turned = {}

        def turn(j):
            if j not in turned:
                value = fields[here, :, pl.ds(j * LANES, LANES)]
                turned[j] = (value, pltpu.roll(value, 1, 1), pltpu.roll(value, LANES - 1, 1))
            return turned[j]

        squares = cross = None
        for j in range(cols):
            part = pl.ds(j * LANES, LANES)
            value, right_by, left_by = turn(j)
            before = turn(j - 1)[1] if j > 0 else 0.0
            after = turn(j + 1)[2] if j < cols - 1 else 0.0
            beside = (jnp.where(at_first, before, right_by) + jnp.where(at_last, after, left_by)
                      + (fields[here - 1, :, part] + fields[here + 1, :, part]))
            result = 0.5 * beside
            if old is not None:
                result = result - fields[old, :, part]
            if keep is not None:
                result = result * keep
            fields[new, :, part] = result
            if gram:
                squares = value * value if squares is None else squares + value * value
                cross = value * result if cross is None else cross + value * result
        if gram:
            grams[2 * level - 2] += squares
            grams[2 * level - 1] += cross

    def inner(level, start):
        def pair(i, carry):
            row = HALO + level + 2 * i
            row_step(level, row, start, True)
            row_step(level, row + 1, start, True)
            return carry
        lax.fori_loop(0, HALO - level, pair, 0)

    inner(1, True)

    def inner_level(level, carry):
        inner(level, False)
        return carry

    lax.fori_loop(2, HALO, inner_level, 0)

    keeps = tuple(jnp.where(has[side], 1.0, 0.0) for side in range(2))

    def both_sides(level, d, start, gram):
        q = level - d
        row_step(level, HALO + q, start, gram, None if gram else keeps[0])
        row_step(level, EXT - HALO - 1 - q, start, gram, None if gram else keeps[1])

    def near_wait(side, d):
        for piece in range(2):
            theirs = HALO - d if side == 0 else EXT - HALO - 1 + d
            part = pl.ds(0, chunk) if piece == 0 else pl.ds(chunk, cells - chunk)
            pltpu.make_async_remote_copy(
                src_ref=fields.at[theirs, :, part], dst_ref=fields.at[theirs, :, part],
                send_sem=near_send.at[side, d - 1, piece], recv_sem=near_recv.at[side, d - 1, piece],
                device_id={"tile": partner[side]}, device_id_type=MESH).wait_recv()

    def far_wait(side, d):
        pltpu.make_async_remote_copy(
            src_ref=far_in.at[side, d - NEAR - 1], dst_ref=far_in.at[side, d - NEAR - 1],
            send_sem=far_send.at[side, d - NEAR - 1], recv_sem=far_recv.at[side, d - NEAR - 1],
            device_id={"tile": partner[side]}, device_id_type=MESH).wait_recv()
        theirs = HALO - d if side == 0 else EXT - HALO - 1 + d
        for group in range(groups):
            both = far_in[side, d - NEAR - 1, group].astype(f32)
            rows = pl.ds(8 * group, 8)
            fields[theirs, rows, pl.ds(0, half)] = both[:8]
            fields[theirs, rows, pl.ds(half, half)] = both[8:]

    def front(d, carry):
        for side in range(2):
            @pl.when(has[side] & (d <= NEAR))
            def _():
                near_wait(side, d)

            @pl.when(has[side] & (d > NEAR))
            def _():
                far_wait(side, d)

        @pl.when(d == 1)
        def _():
            both_sides(1, d, True, True)

        @pl.when(d > 1)
        def _():
            both_sides(1, d, True, False)

        def halo_level(level, c):
            both_sides(level, d, False, False)
            return c

        def own_level(level, c):
            both_sides(level, d, False, True)
            return c

        lax.fori_loop(2, d, halo_level, 0)
        lax.fori_loop(jnp.maximum(d, 2), STEPS + 1, own_level, 0)
        return carry

    lax.fori_loop(1, HALO + 1, front, 0)

    values = [grams[i] for i in range(2 * STEPS)]

    def fold(low, high, shift, lanes):
        kept = low + pltpu.roll(low, LANES - shift, 1)
        if high is None:
            high = jnp.zeros_like(low)
        moved = high + pltpu.roll(high, shift, 1)
        return jnp.where((lanes & shift) == 0, kept, moved)

    shift = LANES // 2
    while len(values) > 1:
        middle = len(values) // 2
        values = [fold(values[i], values[i + middle], shift, lane) for i in range(middle)]
        shift //= 2
    values = [values[0][8 * g:8 * g + 8] for g in range(groups)] + [None] * (8 - groups)
    while len(values) > 1:
        middle = len(values) // 2
        values = [None if values[i] is None else fold(values[i], values[i + middle], shift, lane8)
                  for i in range(middle)]
        shift //= 2
    total = values[0]

    for phase, (stride, size) in enumerate(dims):
        place = places[phase]
        gather[phase, place] = total
        copies = []
        for step in range(1, size):
            there = tile + (lax.rem(place + step, size) - place) * stride
            copy = pltpu.make_async_remote_copy(
                src_ref=gather.at[phase, place], dst_ref=gather.at[phase, place],
                send_sem=red_send.at[phase, step - 1], recv_sem=red_recv.at[phase, step - 1],
                device_id={"tile": there}, device_id_type=MESH)
            copy.start()
            copies.append(copy)
        for copy in copies:
            copy.wait_recv()
        total = gather[phase, 0]
        for i in range(1, size):
            total = total + gather[phase, i]

    dots = [total if i == 0 else pltpu.roll(total, LANES - 8 * i, 1) for i in range(2 * STEPS)]
    moments = dots[:2]
    for i in range(2, 2 * STEPS):
        moments.append(dots[i] - dots[i - 2])
    zero = jnp.zeros_like(total)
    half_scale = 0.5 * scale
    r_mom, p_mom = list(moments), list(moments)
    r_co, p_co, x_co = [zero + 1.0], [zero + 1.0], []
    squares = moments[0]

    def add(items):
        items = list(items)
        while len(items) > 1:
            items = [items[i] + items[i + 1] if i + 1 < len(items) else items[i]
                     for i in range(0, len(items), 2)]
        return items[0]

    for step in range(STEPS):
        through = []
        for i in range(len(p_mom) - 1):
            around = p_mom[i + 1] if i == 0 else p_mom[i - 1] + p_mom[i + 1]
            through.append(p_mom[i] - half_scale * around)
        alpha = squares / add(p_co[i] * through[i] for i in range(step + 1))
        x_co = [x_co[i] + alpha * p_co[i] if i < len(x_co) else alpha * p_co[i] for i in range(step + 1)]
        grown = []
        for i in range(step + 2):
            terms = [p_co[k] for k in (i - 1, i + 1) if 0 <= k <= step]
            moved = p_co[i] if i <= step else zero
            if terms:
                moved = moved - half_scale * add(terms)
            grown.append(r_co[i] - alpha * moved if i < len(r_co) else -(alpha * moved))
        r_co = grown
        if step == STEPS - 1:
            break
        r_mom = [r_mom[i] - alpha * through[i] for i in range(len(through))]
        fresh = add(r_co[i] * r_mom[i] for i in range(step + 2))
        beta = fresh / squares
        squares = fresh
        p_co = [r_co[i] + beta * p_co[i] if i <= step else r_co[i] for i in range(step + 2)]
        p_mom = [r_mom[i] + beta * p_mom[i] for i in range(len(r_mom))]

    for i, value in enumerate(x_co + r_co):
        for group in range(groups):
            coef[i, pl.ds(8 * group, 8), :] = jnp.broadcast_to(value[:, group:group + 1], (8, LANES))

    def out_copy(which, row):
        source = fields.at[flat(7 + which, HALO + row)]
        target = (sol_hbm, res_hbm)[which].at[:, row, :]
        return pltpu.make_async_copy(source, target, out_sem.at[which, row])

    def combine(pair, carry):
        def one_group(group, c):
            rows = pl.ds(pl.multiple_of(8 * group, 8), 8)
            factors = [coef[i, rows, :] for i in range(2 * STEPS + 1)]
            for more in range(2):
                row = HALO + 2 * pair + more
                for j in range(cols):
                    part = pl.ds(j * LANES, LANES)
                    parts = [fields[flat(k, row), rows, part] for k in range(STEPS + 1)]
                    sol = add(factors[k] * parts[k] for k in range(STEPS))
                    res = add(factors[STEPS + k] * parts[k] for k in range(STEPS + 1))
                    fields[flat(7, row), rows, part] = sol
                    fields[flat(8, row), rows, part] = res
            return c
        lax.fori_loop(0, groups, one_group, 0)
        for more in range(2):
            for which in range(2):
                out_copy(which, 2 * pair + more).start()
        return carry

    lax.fori_loop(0, ROWS // 2, combine, 0)

    for send in sends:
        send.wait_send()
    for side in range(2):
        @pl.when(has[side])
        def _():
            for d in range(1, NEAR + 1):
                for piece in range(2):
                    near_copy(side, d, piece).wait_send()
            for d in range(NEAR + 1, HALO + 1):
                far_copy(side, d).wait_send()
    for phase, (stride, size) in enumerate(dims):
        for step in range(1, size):
            pltpu.make_async_remote_copy(
                src_ref=gather.at[phase, places[phase]], dst_ref=gather.at[phase, places[phase]],
                send_sem=red_send.at[phase, step - 1], recv_sem=red_recv.at[phase, step - 1],
                device_id={"tile": tile}, device_id_type=MESH).wait_send()

    def drain(row, carry):
        for which in range(2):
            out_copy(which, row).wait()
        return carry

    lax.fori_loop(0, ROWS, drain, 0)


def shards(dims, increments, projection, helmholtz):
    levels, rows, cells = increments.shape
    modes = projection.shape[0] // 2
    groups = modes // 8
    out = jax.ShapeDtypeStruct((modes, rows, cells), jnp.float32)
    longest = max(size for _, size in dims)
    hbm = pl.BlockSpec(memory_space=pl.ANY)
    dma = pltpu.SemaphoreType.DMA
    return pl.pallas_call(
        functools.partial(kernel, dims),
        out_shape=(out, out),
        in_specs=[hbm, pl.BlockSpec(memory_space=pltpu.VMEM), pl.BlockSpec(memory_space=pltpu.SMEM)],
        out_specs=(hbm, hbm),
        scratch_shapes=[
            pltpu.VMEM((FLAT, modes, cells), jnp.float32),
            pltpu.VMEM((levels, rows, cells), jnp.bfloat16),
            pltpu.VMEM((levels, rows, cells), jnp.bfloat16),
            pltpu.VMEM((2, rows * modes, rows * levels), jnp.bfloat16),
            pltpu.VMEM((2 * STEPS, modes, LANES), jnp.float32),
            pltpu.VMEM((2, HALO - NEAR, groups, 16, cells // 2), jnp.bfloat16),
            pltpu.VMEM((2, HALO - NEAR, groups, 16, cells // 2), jnp.bfloat16),
            pltpu.VMEM((2 * STEPS + 1, modes, LANES), jnp.float32),
            pltpu.VMEM((len(dims), longest, 8, LANES), jnp.float32),
            dma((4,)), dma((4,)), dma((4,)),
            dma((2, NEAR, 2)), dma((2, NEAR, 2)),
            dma((2, HALO - NEAR)), dma((2, HALO - NEAR)),
            dma((len(dims), longest - 1)), dma((len(dims), longest - 1)),
            dma((2, ROWS)),
        ],
        compiler_params=pltpu.CompilerParams(
            collective_id=0, has_side_effects=True, vmem_limit_bytes=60 * 1024 * 1024),
    )(increments, projection, helmholtz)


def solution(mesh):
    tiles = mesh.shape["tile"]
    dims = ((1, 4), (4, 4), (16, 4)) if tiles == 64 else ((1, 2), (2, 2), (4, 2))
    in_specs = (P("lev", "tile", None), P(), P("lev"))
    out_specs = (P("lev", "tile", None), P("lev", "tile", None))
    return jax.shard_map(functools.partial(shards, dims), mesh=mesh, in_specs=in_specs,
                         out_specs=out_specs, check_vma=False)
```

```python
import functools

import jax
import jax.numpy as jnp
from jax import lax
from jax.experimental import pallas as pl
from jax.experimental.pallas import tpu as pltpu
from jax.sharding import PartitionSpec as P

STEPS = 8
ROWS = 16
HALO = 8
EXT = ROWS + 2 * HALO
NEAR = 4
LANES = 128
MESH = pl.DeviceIdType.MESH


def kernel(dims, inc_hbm, proj_ref, helm_ref, sol_hbm, res_hbm,
           inc_own, inc_far, kron, grams, far_out, far_in, coef, gather, sol_rows, res_rows,
           lev_send, lev_recv, load_sem, near_send, near_recv, far_send, far_recv,
           red_send, red_recv, out_sem, *fields):
    tile = lax.axis_index("tile")
    lev = lax.axis_index("lev")
    tiles = lax.axis_size("tile")
    levels, _, cells = inc_own.shape
    modes = fields[0].shape[1]
    groups = modes // 8
    chunk = cells // 4
    cols = cells // LANES
    other = 1 - lev
    has = (tile > 0, tile < tiles - 1)
    partner = (tile - 1, tile + 1)
    f32 = jnp.float32

    loads = []
    for c in range(4):
        part = pl.ds(c * chunk, chunk)
        load = pltpu.make_async_copy(inc_hbm.at[:, :, part], inc_own.at[:, :, part], load_sem.at[c])
        load.start()
        loads.append(load)

    barrier = pltpu.get_barrier_semaphore()
    pl.semaphore_signal(barrier, inc=1, device_id={"lev": other}, device_id_type=MESH)
    for side in range(2):
        there = lax.rem(tile + (tiles - 1 if side == 0 else 1), tiles)
        pl.semaphore_signal(barrier, inc=1, device_id={"tile": there}, device_id_type=MESH)
    places = []
    for stride, size in dims:
        place = lax.rem(lax.div(tile, stride), size)
        places.append(place)
        for step in range(1, size):
            there = tile + (lax.rem(place + step, size) - place) * stride
            pl.semaphore_signal(barrier, inc=1, device_id={"tile": there}, device_id_type=MESH)
    pl.semaphore_wait(barrier, 3 + sum(size - 1 for _, size in dims))

    sends = []
    for c in range(4):
        part = pl.ds(c * chunk, chunk)
        send = pltpu.make_async_remote_copy(
            src_ref=inc_hbm.at[:, :, part], dst_ref=inc_far.at[:, :, part],
            send_sem=lev_send.at[c], recv_sem=lev_recv.at[c],
            device_id={"lev": other}, device_id_type=MESH)
        send.start()
        sends.append(send)

    wide = levels * ROWS
    table = proj_ref[...]
    at_row = lax.broadcasted_iota(jnp.int32, (modes, wide), 1) % ROWS
    of_level = (lax.broadcasted_iota(jnp.int32, (2 * levels, wide), 0)
                - lax.broadcasted_iota(jnp.int32, (2 * levels, wide), 1) // ROWS)
    for half in range(2):
        first_level = (lev if half == 0 else other) * levels
        spread = jnp.where(of_level == first_level, 1.0, 0.0).astype(jnp.bfloat16)
        repeated = lax.dot_general(table, spread, (((0,), (0,)), ((), ())), preferred_element_type=f32)
        repeated = jnp.where(lev == 0, repeated[:modes], repeated[modes:])
        for pair in range(ROWS // 2):
            both = jnp.concatenate([
                jnp.where(at_row == 2 * pair, repeated, 0.0),
                jnp.where(at_row == 2 * pair + 1, repeated, 0.0)], axis=0)
            kron[half, pl.ds(2 * modes * pair, 2 * modes), :] = both.astype(jnp.bfloat16)

    lane8 = lax.broadcasted_iota(jnp.int32, (8, LANES), 1)
    sub8 = lax.broadcasted_iota(jnp.int32, (8, LANES), 0)
    shifts = jnp.zeros((8, LANES), f32)
    for mode in range(modes):
        shifts = jnp.where((lane8 == mode // 8) & (sub8 == mode % 8), helm_ref[mode], shifts)
    scale = 4.0 / (4.0 + shifts)

    for side, base in ((0, 0), (1, EXT - HALO)):
        @pl.when(jnp.logical_not(has[side]))
        def _():
            def clear(row, carry):
                fields[0][row + base] = jnp.zeros((modes, cells), f32)
                return carry
            lax.fori_loop(0, HALO, clear, 0)
    grams[...] = jnp.zeros_like(grams)

    for c in range(4):
        loads[c].wait()
        part = pl.ds(c * chunk, chunk)
        first = jnp.dot(kron[0], inc_own[:, :, part].reshape(wide, chunk), preferred_element_type=f32)
        fields[0][pl.ds(HALO, ROWS), :, part] = first.reshape(ROWS, modes, chunk)

    def near_copy(side, d, piece):
        mine = HALO + d - 1 if side == 0 else EXT - HALO - d
        theirs = EXT - HALO - 1 + d if side == 0 else HALO - d
        part = pl.ds(0, chunk) if piece == 0 else pl.ds(chunk, cells - chunk)
        return pltpu.make_async_remote_copy(
            src_ref=fields[0].at[mine, :, part], dst_ref=fields[0].at[theirs, :, part],
            send_sem=near_send.at[side, d - 1, piece], recv_sem=near_recv.at[1 - side, d - 1, piece],
            device_id={"tile": partner[side]}, device_id_type=MESH)

    def far_copy(side, d):
        return pltpu.make_async_remote_copy(
            src_ref=far_out.at[side, d - NEAR - 1], dst_ref=far_in.at[1 - side, d - NEAR - 1],
            send_sem=far_send.at[side, d - NEAR - 1], recv_sem=far_recv.at[1 - side, d - NEAR - 1],
            device_id={"tile": partner[side]}, device_id_type=MESH)

    for c in range(4):
        sends[c].wait_recv()
        part = pl.ds(c * chunk, chunk)
        second = jnp.dot(kron[1], inc_far[:, :, part].reshape(wide, chunk), preferred_element_type=f32)
        fields[0][pl.ds(HALO, ROWS), :, part] += second.reshape(ROWS, modes, chunk)
        if c in (0, 3):
            for d in range(1, NEAR + 1):
                for side in range(2):
                    @pl.when(has[side])
                    def _():
                        near_copy(side, d, 0 if c == 0 else 1).start()
    half = cells // 2
    for d in range(NEAR + 1, HALO + 1):
        for side in range(2):
            mine = HALO + d - 1 if side == 0 else EXT - HALO - d
            for group in range(groups):
                rows = pl.ds(8 * group, 8)
                both = jnp.concatenate(
                    [fields[0][mine, rows, pl.ds(0, half)], fields[0][mine, rows, pl.ds(half, half)]], axis=0)
                far_out[side, d - NEAR - 1, group] = both.astype(jnp.bfloat16)

            @pl.when(has[side])
            def _():
                far_copy(side, d).start()

    lane = lax.broadcasted_iota(jnp.int32, (modes, LANES), 1)
    at_first, at_last = lane == 0, lane == LANES - 1

    def row_step(level, row, keep=None, weight=None):
        source, new = fields[level - 1], fields[level]
        here, there = row - (level - 1), row - level
        turned = {}

        def turn(j):
            if j not in turned:
                value = source[here, :, pl.ds(j * LANES, LANES)]
                turned[j] = (value, pltpu.roll(value, 1, 1), pltpu.roll(value, LANES - 1, 1))
            return turned[j]

        squares = cross = None
        for j in range(cols):
            part = pl.ds(j * LANES, LANES)
            value, right_by, left_by = turn(j)
            before = turn(j - 1)[1] if j > 0 else 0.0
            after = turn(j + 1)[2] if j < cols - 1 else 0.0
            beside = (jnp.where(at_first, before, right_by) + jnp.where(at_last, after, left_by)
                      + (source[here - 1, :, part] + source[here + 1, :, part]))
            result = 0.5 * beside
            if level > 1:
                result = result - fields[level - 2][row - (level - 2), :, part]
            if keep is not None:
                result = result * keep
            new[there, :, part] = result
            squares = value * value if squares is None else squares + value * value
            cross = value * result if cross is None else cross + value * result
        if weight is not None:
            squares, cross = squares * weight, cross * weight
        grams[2 * level - 2] += squares
        grams[2 * level - 1] += cross

    for level in range(1, HALO):
        def pair(i, carry):
            row_step(level, HALO + level + 2 * i)
            row_step(level, HALO + level + 2 * i + 1)
            return carry
        lax.fori_loop(0, HALO - level, pair, 0)

    keeps = tuple(jnp.where(has[side], 1.0, 0.0) for side in range(2))

    def near_wait(side, d):
        for piece in range(2):
            theirs = HALO - d if side == 0 else EXT - HALO - 1 + d
            part = pl.ds(0, chunk) if piece == 0 else pl.ds(chunk, cells - chunk)
            pltpu.make_async_remote_copy(
                src_ref=fields[0].at[theirs, :, part], dst_ref=fields[0].at[theirs, :, part],
                send_sem=near_send.at[side, d - 1, piece], recv_sem=near_recv.at[side, d - 1, piece],
                device_id={"tile": partner[side]}, device_id_type=MESH).wait_recv()

    def far_wait(side, d):
        pltpu.make_async_remote_copy(
            src_ref=far_in.at[side, d - NEAR - 1], dst_ref=far_in.at[side, d - NEAR - 1],
            send_sem=far_send.at[side, d - NEAR - 1], recv_sem=far_recv.at[side, d - NEAR - 1],
            device_id={"tile": partner[side]}, device_id_type=MESH).wait_recv()
        theirs = HALO - d if side == 0 else EXT - HALO - 1 + d
        for group in range(groups):
            both = far_in[side, d - NEAR - 1, group].astype(f32)
            rows = pl.ds(8 * group, 8)
            fields[0][theirs, rows, pl.ds(0, half)] = both[:8]
            fields[0][theirs, rows, pl.ds(half, half)] = both[8:]

    def front(d, carry):
        for side in range(2):
            @pl.when(has[side] & (d <= NEAR))
            def _():
                near_wait(side, d)

            @pl.when(has[side] & (d > NEAR))
            def _():
                far_wait(side, d)

        top, bottom = HALO - d, EXT - HALO - 1 + d
        for level in range(1, STEPS + 1):
            inside = jnp.where(d <= level, 1.0, 0.0)
            keep = [jnp.maximum(inside, keeps[side]) for side in range(2)]
            row_step(level, top + level, keep[0], inside)
            row_step(level, bottom - level, keep[1], inside)
        return carry

    lax.fori_loop(1, HALO + 1, front, 0)

    values = [grams[i] for i in range(2 * STEPS)]

    def fold(low, high, shift, lanes):
        kept = low + pltpu.roll(low, LANES - shift, 1)
        if high is None:
            high = jnp.zeros_like(low)
        moved = high + pltpu.roll(high, shift, 1)
        return jnp.where((lanes & shift) == 0, kept, moved)

    shift = LANES // 2
    while len(values) > 1:
        middle = len(values) // 2
        values = [fold(values[i], values[i + middle], shift, lane) for i in range(middle)]
        shift //= 2
    values = [values[0][8 * g:8 * g + 8] for g in range(groups)] + [None] * (8 - groups)
    while len(values) > 1:
        middle = len(values) // 2
        values = [None if values[i] is None else fold(values[i], values[i + middle], shift, lane8)
                  for i in range(middle)]
        shift //= 2
    total = values[0]

    for phase, (stride, size) in enumerate(dims):
        place = places[phase]
        gather[phase, place] = total
        copies = []
        for step in range(1, size):
            there = tile + (lax.rem(place + step, size) - place) * stride
            copy = pltpu.make_async_remote_copy(
                src_ref=gather.at[phase, place], dst_ref=gather.at[phase, place],
                send_sem=red_send.at[phase, step - 1], recv_sem=red_recv.at[phase, step - 1],
                device_id={"tile": there}, device_id_type=MESH)
            copy.start()
            copies.append(copy)
        for copy in copies:
            copy.wait_recv()
        total = gather[phase, 0]
        for i in range(1, size):
            total = total + gather[phase, i]

    dots = [total if i == 0 else pltpu.roll(total, LANES - 8 * i, 1) for i in range(2 * STEPS)]
    moments = dots[:2]
    for i in range(2, 2 * STEPS):
        moments.append(dots[i] - dots[i - 2])
    zero = jnp.zeros_like(total)
    half_scale = 0.5 * scale
    r_mom, p_mom = list(moments), list(moments)
    r_co, p_co, x_co = [zero + 1.0], [zero + 1.0], []
    squares = moments[0]

    def add(items):
        items = list(items)
        while len(items) > 1:
            items = [items[i] + items[i + 1] if i + 1 < len(items) else items[i]
                     for i in range(0, len(items), 2)]
        return items[0]

    for step in range(STEPS):
        through = []
        for i in range(len(p_mom) - 1):
            around = p_mom[i + 1] if i == 0 else p_mom[i - 1] + p_mom[i + 1]
            through.append(p_mom[i] - half_scale * around)
        alpha = squares / add(p_co[i] * through[i] for i in range(step + 1))
        x_co = [x_co[i] + alpha * p_co[i] if i < len(x_co) else alpha * p_co[i] for i in range(step + 1)]
        grown = []
        for i in range(step + 2):
            terms = [p_co[k] for k in (i - 1, i + 1) if 0 <= k <= step]
            moved = p_co[i] if i <= step else zero
            if terms:
                moved = moved - half_scale * add(terms)
            grown.append(r_co[i] - alpha * moved if i < len(r_co) else -(alpha * moved))
        r_co = grown
        if step == STEPS - 1:
            break
        r_mom = [r_mom[i] - alpha * through[i] for i in range(len(through))]
        fresh = add(r_co[i] * r_mom[i] for i in range(step + 2))
        beta = fresh / squares
        squares = fresh
        p_co = [r_co[i] + beta * p_co[i] if i <= step else r_co[i] for i in range(step + 2)]
        p_mom = [r_mom[i] + beta * p_mom[i] for i in range(len(r_mom))]

    for i, value in enumerate(x_co + r_co):
        for group in range(groups):
            coef[i, pl.ds(8 * group, 8), :] = jnp.broadcast_to(value[:, group:group + 1], (8, LANES))

    def out_copy(which, row):
        source = (sol_rows, res_rows)[which].at[row]
        target = (sol_hbm, res_hbm)[which].at[:, row, :]
        return pltpu.make_async_copy(source, target, out_sem.at[which, row])

    def combine(pair, carry):
        def one_group(group, c):
            rows = pl.ds(pl.multiple_of(8 * group, 8), 8)
            factors = [coef[i, rows, :] for i in range(2 * STEPS + 1)]
            for more in range(2):
                row = 2 * pair + more
                for j in range(cols):
                    part = pl.ds(j * LANES, LANES)
                    parts = [fields[k][row + HALO - k, rows, part] for k in range(STEPS + 1)]
                    sol = add(factors[k] * parts[k] for k in range(STEPS))
                    res = add(factors[STEPS + k] * parts[k] for k in range(STEPS + 1))
                    sol_rows[row, rows, part] = sol
                    res_rows[row, rows, part] = res
            return c
        lax.fori_loop(0, groups, one_group, 0)
        for more in range(2):
            for which in range(2):
                out_copy(which, 2 * pair + more).start()
        return carry

    lax.fori_loop(0, ROWS // 2, combine, 0)

    for send in sends:
        send.wait_send()
    for side in range(2):
        @pl.when(has[side])
        def _():
            for d in range(1, NEAR + 1):
                for piece in range(2):
                    near_copy(side, d, piece).wait_send()
            for d in range(NEAR + 1, HALO + 1):
                far_copy(side, d).wait_send()
    for phase, (stride, size) in enumerate(dims):
        for step in range(1, size):
            pltpu.make_async_remote_copy(
                src_ref=gather.at[phase, places[phase]], dst_ref=gather.at[phase, places[phase]],
                send_sem=red_send.at[phase, step - 1], recv_sem=red_recv.at[phase, step - 1],
                device_id={"tile": tile}, device_id_type=MESH).wait_send()

    def drain(row, carry):
        for which in range(2):
            out_copy(which, row).wait()
        return carry

    lax.fori_loop(0, ROWS, drain, 0)


def shards(dims, increments, projection, helmholtz):
    levels, rows, cells = increments.shape
    modes = projection.shape[0] // 2
    groups = modes // 8
    out = jax.ShapeDtypeStruct((modes, rows, cells), jnp.float32)
    longest = max(size for _, size in dims)
    hbm = pl.BlockSpec(memory_space=pl.ANY)
    dma = pltpu.SemaphoreType.DMA
    return pl.pallas_call(
        functools.partial(kernel, dims),
        out_shape=(out, out),
        in_specs=[hbm, pl.BlockSpec(memory_space=pltpu.VMEM), pl.BlockSpec(memory_space=pltpu.SMEM)],
        out_specs=(hbm, hbm),
        scratch_shapes=[
            pltpu.VMEM((levels, rows, cells), jnp.bfloat16),
            pltpu.VMEM((levels, rows, cells), jnp.bfloat16),
            pltpu.VMEM((2, rows * modes, rows * levels), jnp.bfloat16),
            pltpu.VMEM((2 * STEPS, modes, LANES), jnp.float32),
            pltpu.VMEM((2, HALO - NEAR, groups, 16, cells // 2), jnp.bfloat16),
            pltpu.VMEM((2, HALO - NEAR, groups, 16, cells // 2), jnp.bfloat16),
            pltpu.VMEM((2 * STEPS + 1, modes, LANES), jnp.float32),
            pltpu.VMEM((len(dims), longest, 8, LANES), jnp.float32),
            pltpu.VMEM((rows, modes, cells), jnp.float32),
            pltpu.VMEM((rows, modes, cells), jnp.float32),
            dma((4,)), dma((4,)), dma((4,)),
            dma((2, NEAR, 2)), dma((2, NEAR, 2)),
            dma((2, HALO - NEAR)), dma((2, HALO - NEAR)),
            dma((len(dims), longest - 1)), dma((len(dims), longest - 1)),
            dma((2, ROWS)),
        ] + [pltpu.VMEM((EXT - 2 * k, modes, cells), jnp.float32) for k in range(STEPS + 1)],
        compiler_params=pltpu.CompilerParams(
            collective_id=0, has_side_effects=True, vmem_limit_bytes=60 * 1024 * 1024),
    )(increments, projection.T, helmholtz)


def solution(mesh):
    tiles = mesh.shape["tile"]
    dims = ((1, 4), (4, 4), (16, 4)) if tiles == 64 else ((1, 2), (2, 2), (4, 2))
    in_specs = (P("lev", "tile", None), P(), P("lev"))
    out_specs = (P("lev", "tile", None), P("lev", "tile", None))
    return jax.shard_map(functools.partial(shards, dims), mesh=mesh, in_specs=in_specs,
                         out_specs=out_specs, check_vma=False)
```

```python
import functools

import jax
import jax.numpy as jnp
from jax import lax
from jax.experimental import pallas as pl
from jax.experimental.pallas import tpu as pltpu
from jax.sharding import PartitionSpec as P

STEPS = 8
ROWS = 16
HALO = 8
EXT = ROWS + 2 * HALO
NEAR = 4
LANES = 128
MESH = pl.DeviceIdType.MESH


def add(items):
    items = list(items)
    while len(items) > 1:
        items = [items[i] + items[i + 1] if i + 1 < len(items) else items[i]
                 for i in range(0, len(items), 2)]
    return items[0]


def kernel(dims, inc_hbm, proj_hbm, helm_hbm, coef, *refs):
    fields = refs[:STEPS + 1]
    (inc_own, inc_far, kron, grams, far_out, far_in, gather,
     lev_send, lev_recv, load_sem, near_send, near_recv, far_send, far_recv,
     red_send, red_recv, proj_ref, helm_ref, small_sem) = refs[STEPS + 1:]
    tile = lax.axis_index("tile")
    lev = lax.axis_index("lev")
    tiles = lax.axis_size("tile")
    levels, _, cells = inc_own.shape
    modes = fields[0].shape[1]
    groups = modes // 8
    chunk = cells // 4
    cols = cells // LANES
    other = 1 - lev
    has = (tile > 0, tile < tiles - 1)
    partner = (tile - 1, tile + 1)
    f32 = jnp.float32

    barrier = pltpu.get_barrier_semaphore()
    pl.semaphore_signal(barrier, inc=1, device_id={"lev": other}, device_id_type=MESH)
    for side in range(2):
        @pl.when(has[side])
        def _():
            pl.semaphore_signal(barrier, inc=1, device_id={"tile": partner[side]}, device_id_type=MESH)
    places = []
    for stride, size in dims:
        place = lax.rem(lax.div(tile, stride), size)
        places.append(place)
        for step in range(1, size):
            there = tile + (lax.rem(place + step, size) - place) * stride
            pl.semaphore_signal(barrier, inc=1, device_id={"tile": there}, device_id_type=MESH)

    loads = []
    for c in range(4):
        part = pl.ds(c * chunk, chunk)
        load = pltpu.make_async_copy(inc_hbm.at[:, :, part], inc_own.at[:, :, part], load_sem.at[c])
        load.start()
        loads.append(load)
    small = (pltpu.make_async_copy(proj_hbm, proj_ref, small_sem.at[0]),
             pltpu.make_async_copy(helm_hbm, helm_ref, small_sem.at[1]))
    for load in small:
        load.start()

    peers = 1 + sum(size - 1 for _, size in dims)
    pl.semaphore_wait(barrier, peers + sum(jnp.where(has[side], 1, 0) for side in range(2)))

    sends = []
    for c in range(4):
        part = pl.ds(c * chunk, chunk)
        send = pltpu.make_async_remote_copy(
            src_ref=inc_hbm.at[:, :, part], dst_ref=inc_far.at[:, :, part],
            send_sem=lev_send.at[c], recv_sem=lev_recv.at[c],
            device_id={"lev": other}, device_id_type=MESH)
        send.start()
        sends.append(send)

    wide = levels * ROWS
    for load in small:
        load.wait()
    table = proj_ref[...]
    at_row = lax.broadcasted_iota(jnp.int32, (modes, wide), 1) % ROWS
    of_level = (lax.broadcasted_iota(jnp.int32, (2 * levels, wide), 0)
                - lax.broadcasted_iota(jnp.int32, (2 * levels, wide), 1) // ROWS)
    for half in range(2):
        first_level = (lev if half == 0 else other) * levels
        spread = jnp.where(of_level == first_level, 1.0, 0.0).astype(jnp.bfloat16)
        repeated = lax.dot_general(table, spread, (((0,), (0,)), ((), ())), preferred_element_type=f32)
        repeated = jnp.where(lev == 0, repeated[:modes], repeated[modes:])
        for pair in range(ROWS // 2):
            both = jnp.concatenate([
                jnp.where(at_row == 2 * pair, repeated, 0.0),
                jnp.where(at_row == 2 * pair + 1, repeated, 0.0)], axis=0)
            kron[half, pl.ds(2 * modes * pair, 2 * modes), :] = both.astype(jnp.bfloat16)

    lane8 = lax.broadcasted_iota(jnp.int32, (8, LANES), 1)
    sub8 = lax.broadcasted_iota(jnp.int32, (8, LANES), 0)
    shifts = jnp.zeros((8, LANES), f32)
    for mode in range(modes):
        shifts = jnp.where((lane8 == mode // 8) & (sub8 == mode % 8), helm_ref[mode], shifts)
    scale = 4.0 / (4.0 + shifts)

    for side, base in ((0, 0), (1, EXT - HALO)):
        @pl.when(jnp.logical_not(has[side]))
        def _():
            def clear(row, carry):
                fields[0][row + base] = jnp.zeros((modes, cells), f32)
                return carry
            lax.fori_loop(0, HALO, clear, 0)
    grams[...] = jnp.zeros_like(grams)

    for c in range(4):
        loads[c].wait()
        part = pl.ds(c * chunk, chunk)
        first = jnp.dot(kron[0], inc_own[:, :, part].reshape(wide, chunk), preferred_element_type=f32)
        fields[0][pl.ds(HALO, ROWS), :, part] = first.reshape(ROWS, modes, chunk)

    def near_copy(side, d, piece):
        mine = HALO + d - 1 if side == 0 else EXT - HALO - d
        theirs = EXT - HALO - 1 + d if side == 0 else HALO - d
        part = pl.ds(0, chunk) if piece == 0 else pl.ds(chunk, cells - chunk)
        return pltpu.make_async_remote_copy(
            src_ref=fields[0].at[mine, :, part], dst_ref=fields[0].at[theirs, :, part],
            send_sem=near_send.at[side, d - 1, piece], recv_sem=near_recv.at[1 - side, d - 1, piece],
            device_id={"tile": partner[side]}, device_id_type=MESH)

    def far_copy(side, d):
        return pltpu.make_async_remote_copy(
            src_ref=far_out.at[side, d - NEAR - 1], dst_ref=far_in.at[1 - side, d - NEAR - 1],
            send_sem=far_send.at[side, d - NEAR - 1], recv_sem=far_recv.at[1 - side, d - NEAR - 1],
            device_id={"tile": partner[side]}, device_id_type=MESH)

    for c in range(4):
        sends[c].wait_recv()
        part = pl.ds(c * chunk, chunk)
        second = jnp.dot(kron[1], inc_far[:, :, part].reshape(wide, chunk), preferred_element_type=f32)
        fields[0][pl.ds(HALO, ROWS), :, part] += second.reshape(ROWS, modes, chunk)
        if c in (0, 3):
            for d in range(1, NEAR + 1):
                for side in range(2):
                    @pl.when(has[side])
                    def _():
                        near_copy(side, d, 0 if c == 0 else 1).start()
    half = cells // 2
    for d in range(NEAR + 1, HALO + 1):
        for side in range(2):
            mine = HALO + d - 1 if side == 0 else EXT - HALO - d
            for group in range(groups):
                rows = pl.ds(8 * group, 8)
                both = jnp.concatenate(
                    [fields[0][mine, rows, pl.ds(0, half)], fields[0][mine, rows, pl.ds(half, half)]], axis=0)
                far_out[side, d - NEAR - 1, group] = both.astype(jnp.bfloat16)

            @pl.when(has[side])
            def _():
                far_copy(side, d).start()

    lane = lax.broadcasted_iota(jnp.int32, (modes, LANES), 1)
    at_first, at_last = lane == 0, lane == LANES - 1

    def row_step(level, row, keep=None, weight=None):
        source, new = fields[level - 1], fields[level]
        here, there = row - (level - 1), row - level
        turned = {}

        def turn(j):
            if j not in turned:
                value = source[here, :, pl.ds(j * LANES, LANES)]
                turned[j] = (value, pltpu.roll(value, 1, 1), pltpu.roll(value, LANES - 1, 1))
            return turned[j]

        squares = cross = None
        for j in range(cols):
            part = pl.ds(j * LANES, LANES)
            value, right_by, left_by = turn(j)
            before = turn(j - 1)[1] if j > 0 else 0.0
            after = turn(j + 1)[2] if j < cols - 1 else 0.0
            beside = (jnp.where(at_first, before, right_by) + jnp.where(at_last, after, left_by)
                      + (source[here - 1, :, part] + source[here + 1, :, part]))
            result = 0.5 * beside
            if level > 1:
                result = result - fields[level - 2][row - (level - 2), :, part]
            if keep is not None:
                result = result * keep
            new[there, :, part] = result
            squares = value * value if squares is None else squares + value * value
            cross = value * result if cross is None else cross + value * result
        if weight is not None:
            squares, cross = squares * weight, cross * weight
        grams[2 * level - 2] += squares
        grams[2 * level - 1] += cross

    for level in range(1, HALO):
        def pair(i, carry):
            row_step(level, HALO + level + 2 * i)
            row_step(level, HALO + level + 2 * i + 1)
            return carry
        lax.fori_loop(0, HALO - level, pair, 0)

    keeps = tuple(jnp.where(has[side], 1.0, 0.0) for side in range(2))

    def near_wait(side, d):
        for piece in range(2):
            theirs = HALO - d if side == 0 else EXT - HALO - 1 + d
            part = pl.ds(0, chunk) if piece == 0 else pl.ds(chunk, cells - chunk)
            pltpu.make_async_remote_copy(
                src_ref=fields[0].at[theirs, :, part], dst_ref=fields[0].at[theirs, :, part],
                send_sem=near_send.at[side, d - 1, piece], recv_sem=near_recv.at[side, d - 1, piece],
                device_id={"tile": partner[side]}, device_id_type=MESH).wait_recv()

    def far_wait(side, d):
        pltpu.make_async_remote_copy(
            src_ref=far_in.at[side, d - NEAR - 1], dst_ref=far_in.at[side, d - NEAR - 1],
            send_sem=far_send.at[side, d - NEAR - 1], recv_sem=far_recv.at[side, d - NEAR - 1],
            device_id={"tile": partner[side]}, device_id_type=MESH).wait_recv()
        theirs = HALO - d if side == 0 else EXT - HALO - 1 + d
        for group in range(groups):
            both = far_in[side, d - NEAR - 1, group].astype(f32)
            rows = pl.ds(8 * group, 8)
            fields[0][theirs, rows, pl.ds(0, half)] = both[:8]
            fields[0][theirs, rows, pl.ds(half, half)] = both[8:]

    def front(d, carry):
        for side in range(2):
            @pl.when(has[side] & (d <= NEAR))
            def _():
                near_wait(side, d)

            @pl.when(has[side] & (d > NEAR))
            def _():
                far_wait(side, d)

        top, bottom = HALO - d, EXT - HALO - 1 + d
        for level in range(1, STEPS + 1):
            inside = jnp.where(d <= level, 1.0, 0.0)
            keep = [jnp.maximum(inside, keeps[side]) for side in range(2)]
            row_step(level, top + level, keep[0], inside)
            row_step(level, bottom - level, keep[1], inside)
        return carry

    lax.fori_loop(1, HALO + 1, front, 0)

    values = [grams[i] for i in range(2 * STEPS)]

    def fold(low, high, shift, lanes):
        kept = low + pltpu.roll(low, LANES - shift, 1)
        if high is None:
            high = jnp.zeros_like(low)
        moved = high + pltpu.roll(high, shift, 1)
        return jnp.where((lanes & shift) == 0, kept, moved)

    shift = LANES // 2
    while len(values) > 1:
        middle = len(values) // 2
        values = [fold(values[i], values[i + middle], shift, lane) for i in range(middle)]
        shift //= 2
    values = [values[0][8 * g:8 * g + 8] for g in range(groups)] + [None] * (8 - groups)
    while len(values) > 1:
        middle = len(values) // 2
        values = [None if values[i] is None else fold(values[i], values[i + middle], shift, lane8)
                  for i in range(middle)]
        shift //= 2
    total = values[0]

    for phase, (stride, size) in enumerate(dims):
        place = places[phase]
        gather[phase, place] = total
        copies = []
        for step in range(1, size):
            there = tile + (lax.rem(place + step, size) - place) * stride
            copy = pltpu.make_async_remote_copy(
                src_ref=gather.at[phase, place], dst_ref=gather.at[phase, place],
                send_sem=red_send.at[phase, step - 1], recv_sem=red_recv.at[phase, step - 1],
                device_id={"tile": there}, device_id_type=MESH)
            copy.start()
            copies.append(copy)
        for copy in copies:
            copy.wait_recv()
        total = gather[phase, 0]
        for i in range(1, size):
            total = total + gather[phase, i]

    dots = [total if i == 0 else pltpu.roll(total, LANES - 8 * i, 1) for i in range(2 * STEPS)]
    moments = dots[:2]
    for i in range(2, 2 * STEPS):
        moments.append(dots[i] - dots[i - 2])
    zero = jnp.zeros_like(total)
    half_scale = 0.5 * scale
    r_mom, p_mom = list(moments), list(moments)
    r_co, p_co, x_co = [zero + 1.0], [zero + 1.0], []
    squares = moments[0]

    for step in range(STEPS):
        through = []
        for i in range(len(p_mom) - 1):
            around = p_mom[i + 1] if i == 0 else p_mom[i - 1] + p_mom[i + 1]
            through.append(p_mom[i] - half_scale * around)
        alpha = squares / add(p_co[i] * through[i] for i in range(step + 1))
        x_co = [x_co[i] + alpha * p_co[i] if i < len(x_co) else alpha * p_co[i] for i in range(step + 1)]
        grown = []
        for i in range(step + 2):
            terms = [p_co[k] for k in (i - 1, i + 1) if 0 <= k <= step]
            moved = p_co[i] if i <= step else zero
            if terms:
                moved = moved - half_scale * add(terms)
            grown.append(r_co[i] - alpha * moved if i < len(r_co) else -(alpha * moved))
        r_co = grown
        if step == STEPS - 1:
            break
        r_mom = [r_mom[i] - alpha * through[i] for i in range(len(through))]
        fresh = add(r_co[i] * r_mom[i] for i in range(step + 2))
        beta = fresh / squares
        squares = fresh
        p_co = [r_co[i] + beta * p_co[i] if i <= step else r_co[i] for i in range(step + 2)]
        p_mom = [r_mom[i] + beta * p_mom[i] for i in range(len(r_mom))]

    for i, value in enumerate(x_co + r_co):
        for group in range(groups):
            coef[i, pl.ds(8 * group, 8), :] = jnp.broadcast_to(value[:, group:group + 1], (8, LANES))

    for send in sends:
        send.wait_send()
    for side in range(2):
        @pl.when(has[side])
        def _():
            for d in range(1, NEAR + 1):
                for piece in range(2):
                    near_copy(side, d, piece).wait_send()
            for d in range(NEAR + 1, HALO + 1):
                far_copy(side, d).wait_send()
    for phase, (stride, size) in enumerate(dims):
        for step in range(1, size):
            pltpu.make_async_remote_copy(
                src_ref=gather.at[phase, places[phase]], dst_ref=gather.at[phase, places[phase]],
                send_sem=red_send.at[phase, step - 1], recv_sem=red_recv.at[phase, step - 1],
                device_id={"tile": tile}, device_id_type=MESH).wait_send()


def combine_kernel(*refs):
    coef, fields = refs[0], refs[1:STEPS + 2]
    sol_hbm, res_hbm, sol_rows, res_rows, out_sem = refs[STEPS + 2:]
    groups = fields[0].shape[1] // 8
    cols = fields[0].shape[2] // LANES

    def out_copy(which, row):
        source = (sol_rows, res_rows)[which].at[row]
        target = (sol_hbm, res_hbm)[which].at[:, row, :]
        return pltpu.make_async_copy(source, target, out_sem.at[which, row])

    def combine(pair, carry):
        def one_group(group, c):
            rows = pl.ds(pl.multiple_of(8 * group, 8), 8)
            factors = [coef[i, rows, :] for i in range(2 * STEPS + 1)]
            for more in range(2):
                row = 2 * pair + more
                for j in range(cols):
                    part = pl.ds(j * LANES, LANES)
                    parts = [fields[k][row + HALO - k, rows, part] for k in range(STEPS + 1)]
                    sol = add(factors[k] * parts[k] for k in range(STEPS))
                    res = add(factors[STEPS + k] * parts[k] for k in range(STEPS + 1))
                    sol_rows[row, rows, part] = sol
                    res_rows[row, rows, part] = res
            return c
        lax.fori_loop(0, groups, one_group, 0)
        for more in range(2):
            for which in range(2):
                out_copy(which, 2 * pair + more).start()
        return carry

    lax.fori_loop(0, ROWS // 2, combine, 0)

    def drain(row, carry):
        for which in range(2):
            out_copy(which, row).wait()
        return carry

    lax.fori_loop(0, ROWS, drain, 0)


def shards(dims, increments, projection, helmholtz):
    levels, rows, cells = increments.shape
    modes = projection.shape[0] // 2
    groups = modes // 8
    out = jax.ShapeDtypeStruct((modes, rows, cells), jnp.float32)
    longest = max(size for _, size in dims)
    hbm = pl.BlockSpec(memory_space=pltpu.HBM)
    dma = pltpu.SemaphoreType.DMA
    vmem = pl.BlockSpec(memory_space=pltpu.VMEM)
    kept = [pltpu.VMEM((2 * STEPS + 1, modes, LANES), jnp.float32)]
    kept += [pltpu.VMEM((EXT - 2 * k, modes, cells), jnp.float32) for k in range(STEPS + 1)]
    fields = pl.pallas_call(
        functools.partial(kernel, dims),
        out_shape=tuple(kept),
        in_specs=[hbm] * 3,
        out_specs=(vmem,) * len(kept),
        scratch_shapes=[
            pltpu.VMEM((levels, rows, cells), jnp.bfloat16),
            pltpu.VMEM((levels, rows, cells), jnp.bfloat16),
            pltpu.VMEM((2, rows * modes, rows * levels), jnp.bfloat16),
            pltpu.VMEM((2 * STEPS, modes, LANES), jnp.float32),
            pltpu.VMEM((2, HALO - NEAR, groups, 16, cells // 2), jnp.bfloat16),
            pltpu.VMEM((2, HALO - NEAR, groups, 16, cells // 2), jnp.bfloat16),
            pltpu.VMEM((len(dims), longest, 8, LANES), jnp.float32),
            dma((4,)), dma((4,)), dma((4,)),
            dma((2, NEAR, 2)), dma((2, NEAR, 2)),
            dma((2, HALO - NEAR)), dma((2, HALO - NEAR)),
            dma((len(dims), longest - 1)), dma((len(dims), longest - 1)),
            pltpu.VMEM((2 * levels, 2 * modes), jnp.bfloat16), pltpu.SMEM((modes,), jnp.float32), dma((2,)),
        ],
        compiler_params=pltpu.CompilerParams(
            collective_id=0, has_side_effects=True, vmem_limit_bytes=14 * 1024 * 1024),
    )(*(pltpu.with_memory_space_constraint(x, pltpu.HBM) for x in (increments, projection.T, helmholtz)))
    return pl.pallas_call(
        combine_kernel,
        out_shape=(out, out),
        in_specs=[vmem] * len(kept),
        out_specs=(hbm, hbm),
        scratch_shapes=[
            pltpu.VMEM((rows, modes, cells), jnp.float32),
            pltpu.VMEM((rows, modes, cells), jnp.float32),
            dma((2, ROWS)),
        ],
        compiler_params=pltpu.CompilerParams(vmem_limit_bytes=10 * 1024 * 1024),
    )(*fields)


def solution(mesh):
    tiles = mesh.shape["tile"]
    dims = ((1, 4), (4, 4), (16, 4)) if tiles == 64 else ((1, 2), (2, 2), (4, 2))
    in_specs = (P("lev", "tile", None), P(), P("lev"))
    out_specs = (P("lev", "tile", None), P("lev", "tile", None))
    return jax.shard_map(functools.partial(shards, dims), mesh=mesh, in_specs=in_specs,
                         out_specs=out_specs, check_vma=False)
```

```python
import functools

import jax
import jax.numpy as jnp
from jax import lax
from jax.experimental import pallas as pl
from jax.experimental.pallas import tpu as pltpu
from jax.sharding import PartitionSpec as P

STEPS = 8
ROWS = 16
HALO = 8
EXT = ROWS + 2 * HALO
NEAR = 4
LANES = 128
MESH = pl.DeviceIdType.MESH


def add(items):
    items = list(items)
    while len(items) > 1:
        items = [items[i] + items[i + 1] if i + 1 < len(items) else items[i]
                 for i in range(0, len(items), 2)]
    return items[0]


def kernel(dims, inc_hbm, proj_hbm, helm_hbm, coef, *refs):
    fields = refs[:STEPS + 1]
    (inc_own, inc_far, kron, grams, far_out, far_in, gather,
     lev_send, lev_recv, load_sem, near_send, near_recv, far_send, far_recv,
     red_send, red_recv, proj_ref, helm_ref, small_sem, relay_sem) = refs[STEPS + 1:]
    tile = lax.axis_index("tile")
    lev = lax.axis_index("lev")
    tiles = lax.axis_size("tile")
    levels, _, cells = inc_own.shape
    modes = fields[0].shape[1]
    groups = modes // 8
    chunk = cells // 4
    cols = cells // LANES
    other = 1 - lev
    has = (tile > 0, tile < tiles - 1)
    partner = (tile - 1, tile + 1)
    f32 = jnp.float32

    barrier = pltpu.get_barrier_semaphore()
    pl.semaphore_signal(barrier, inc=1, device_id={"lev": other}, device_id_type=MESH)
    block = dims[2][0]
    corner = dims[1][0] * (dims[1][1] - 1)
    spot = lax.rem(tile, block)
    close = (spot != 0, spot != block - 1)
    for side in range(2):
        @pl.when(close[side])
        def _():
            pl.semaphore_signal(barrier, inc=1, device_id={"tile": partner[side]}, device_id_type=MESH)
    places = []
    for stride, size in dims:
        place = lax.rem(lax.div(tile, stride), size)
        places.append(place)
        for step in range(1, size):
            there = tile + (lax.rem(place + step, size) - place) * stride
            pl.semaphore_signal(barrier, inc=1, device_id={"tile": there}, device_id_type=MESH)

    loads = []
    for c in range(4):
        part = pl.ds(c * chunk, chunk)
        load = pltpu.make_async_copy(inc_hbm.at[:, :, part], inc_own.at[:, :, part], load_sem.at[c])
        load.start()
        loads.append(load)
    small = (pltpu.make_async_copy(proj_hbm, proj_ref, small_sem.at[0]),
             pltpu.make_async_copy(helm_hbm, helm_ref, small_sem.at[1]))
    for load in small:
        load.start()

    peers = 1 + sum(size - 1 for _, size in dims)
    pl.semaphore_wait(barrier, peers + sum(jnp.where(close[side], 1, 0) for side in range(2)))

    sends = []
    for c in range(4):
        part = pl.ds(c * chunk, chunk)
        send = pltpu.make_async_remote_copy(
            src_ref=inc_hbm.at[:, :, part], dst_ref=inc_far.at[:, :, part],
            send_sem=lev_send.at[c], recv_sem=lev_recv.at[c],
            device_id={"lev": other}, device_id_type=MESH)
        send.start()
        sends.append(send)

    inner = tile + block < tiles
    ends = ((spot == block - 1) & inner, (spot == 0) & (tile > 0))
    relays = ((spot == corner) & inner, (spot == 0) & inner)

    def pass_on(condition, arrives, leaves, there):
        @pl.when(condition)
        def _():
            if arrives is not None:
                pl.semaphore_wait(relay_sem.at[arrives], 1)
            if leaves is not None:
                pl.semaphore_signal(relay_sem.at[leaves], inc=1, device_id={"tile": there}, device_id_type=MESH)

    pass_on(ends[1], None, 0, tile - block)
    pass_on(ends[0], None, 3, tile - (block - 1 - corner))

    wide = levels * ROWS
    for load in small:
        load.wait()
    table = proj_ref[...]
    at_row = lax.broadcasted_iota(jnp.int32, (modes, wide), 1) % ROWS
    of_level = (lax.broadcasted_iota(jnp.int32, (2 * levels, wide), 0)
                - lax.broadcasted_iota(jnp.int32, (2 * levels, wide), 1) // ROWS)
    for half in range(2):
        first_level = (lev if half == 0 else other) * levels
        spread = jnp.where(of_level == first_level, 1.0, 0.0).astype(jnp.bfloat16)
        repeated = lax.dot_general(table, spread, (((0,), (0,)), ((), ())), preferred_element_type=f32)
        repeated = jnp.where(lev == 0, repeated[:modes], repeated[modes:])
        for pair in range(ROWS // 2):
            both = jnp.concatenate([
                jnp.where(at_row == 2 * pair, repeated, 0.0),
                jnp.where(at_row == 2 * pair + 1, repeated, 0.0)], axis=0)
            kron[half, pl.ds(2 * modes * pair, 2 * modes), :] = both.astype(jnp.bfloat16)

    pass_on(relays[1], 0, 1, tile + corner)
    pass_on(relays[0], 3, 4, tile - corner)

    lane8 = lax.broadcasted_iota(jnp.int32, (8, LANES), 1)
    sub8 = lax.broadcasted_iota(jnp.int32, (8, LANES), 0)
    shifts = jnp.zeros((8, LANES), f32)
    for mode in range(modes):
        shifts = jnp.where((lane8 == mode // 8) & (sub8 == mode % 8), helm_ref[mode], shifts)
    scale = 4.0 / (4.0 + shifts)

    for side, base in ((0, 0), (1, EXT - HALO)):
        @pl.when(jnp.logical_not(has[side]))
        def _():
            def clear(row, carry):
                fields[0][row + base] = jnp.zeros((modes, cells), f32)
                return carry
            lax.fori_loop(0, HALO, clear, 0)
    grams[...] = jnp.zeros_like(grams)

    for c in range(4):
        loads[c].wait()
        part = pl.ds(c * chunk, chunk)
        first = jnp.dot(kron[0], inc_own[:, :, part].reshape(wide, chunk), preferred_element_type=f32)
        fields[0][pl.ds(HALO, ROWS), :, part] = first.reshape(ROWS, modes, chunk)

    pass_on(relays[0], 1, 2, tile + (block - 1 - corner))
    pass_on(relays[1], 4, 5, tile + block)

    def near_copy(side, d, piece):
        mine = HALO + d - 1 if side == 0 else EXT - HALO - d
        theirs = EXT - HALO - 1 + d if side == 0 else HALO - d
        part = pl.ds(0, chunk) if piece == 0 else pl.ds(chunk, cells - chunk)
        return pltpu.make_async_remote_copy(
            src_ref=fields[0].at[mine, :, part], dst_ref=fields[0].at[theirs, :, part],
            send_sem=near_send.at[side, d - 1, piece], recv_sem=near_recv.at[1 - side, d - 1, piece],
            device_id={"tile": partner[side]}, device_id_type=MESH)

    def far_copy(side, d):
        return pltpu.make_async_remote_copy(
            src_ref=far_out.at[side, d - NEAR - 1], dst_ref=far_in.at[1 - side, d - NEAR - 1],
            send_sem=far_send.at[side, d - NEAR - 1], recv_sem=far_recv.at[1 - side, d - NEAR - 1],
            device_id={"tile": partner[side]}, device_id_type=MESH)

    for c in range(4):
        sends[c].wait_recv()
        part = pl.ds(c * chunk, chunk)
        second = jnp.dot(kron[1], inc_far[:, :, part].reshape(wide, chunk), preferred_element_type=f32)
        fields[0][pl.ds(HALO, ROWS), :, part] += second.reshape(ROWS, modes, chunk)
        if c == 0:
            pass_on(ends[0], 2, None, None)
            pass_on(ends[1], 5, None, None)
        if c in (0, 3):
            for d in range(1, NEAR + 1):
                for side in range(2):
                    @pl.when(has[side])
                    def _():
                        near_copy(side, d, 0 if c == 0 else 1).start()
    half = cells // 2
    for d in range(NEAR + 1, HALO + 1):
        for side in range(2):
            mine = HALO + d - 1 if side == 0 else EXT - HALO - d
            for group in range(groups):
                rows = pl.ds(8 * group, 8)
                both = jnp.concatenate(
                    [fields[0][mine, rows, pl.ds(0, half)], fields[0][mine, rows, pl.ds(half, half)]], axis=0)
                far_out[side, d - NEAR - 1, group] = both.astype(jnp.bfloat16)

            @pl.when(has[side])
            def _():
                far_copy(side, d).start()

    lane = lax.broadcasted_iota(jnp.int32, (modes, LANES), 1)
    at_first, at_last = lane == 0, lane == LANES - 1

    def row_step(level, row, keep=None, gram=True):
        source, new = fields[level - 1], fields[level]
        here, there = row - (level - 1), row - level
        turned = {}

        def turn(j):
            if j not in turned:
                value = source[here, :, pl.ds(j * LANES, LANES)]
                turned[j] = (value, pltpu.roll(value, 1, 1), pltpu.roll(value, LANES - 1, 1))
            return turned[j]

        squares = cross = None
        for j in range(cols):
            part = pl.ds(j * LANES, LANES)
            value, right_by, left_by = turn(j)
            before = turn(j - 1)[1] if j > 0 else 0.0
            after = turn(j + 1)[2] if j < cols - 1 else 0.0
            beside = (jnp.where(at_first, before, right_by) + jnp.where(at_last, after, left_by)
                      + (source[here - 1, :, part] + source[here + 1, :, part]))
            result = 0.5 * beside
            if level > 1:
                result = result - fields[level - 2][row - (level - 2), :, part]
            if keep is not None:
                result = result * keep
            new[there, :, part] = result
            if gram:
                squares = value * value if squares is None else squares + value * value
                cross = value * result if cross is None else cross + value * result
        if gram:
            grams[2 * level - 2] += squares
            grams[2 * level - 1] += cross

    for level in range(1, HALO):
        def pair(i, carry):
            row_step(level, HALO + level + 2 * i)
            row_step(level, HALO + level + 2 * i + 1)
            return carry
        lax.fori_loop(0, HALO - level, pair, 0)

    keeps = tuple(jnp.where(has[side], 1.0, 0.0) for side in range(2))

    def near_wait(side, d):
        for piece in range(2):
            theirs = HALO - d if side == 0 else EXT - HALO - 1 + d
            part = pl.ds(0, chunk) if piece == 0 else pl.ds(chunk, cells - chunk)
            pltpu.make_async_remote_copy(
                src_ref=fields[0].at[theirs, :, part], dst_ref=fields[0].at[theirs, :, part],
                send_sem=near_send.at[side, d - 1, piece], recv_sem=near_recv.at[side, d - 1, piece],
                device_id={"tile": partner[side]}, device_id_type=MESH).wait_recv()

    def far_wait(side, d):
        pltpu.make_async_remote_copy(
            src_ref=far_in.at[side, d - NEAR - 1], dst_ref=far_in.at[side, d - NEAR - 1],
            send_sem=far_send.at[side, d - NEAR - 1], recv_sem=far_recv.at[side, d - NEAR - 1],
            device_id={"tile": partner[side]}, device_id_type=MESH).wait_recv()
        theirs = HALO - d if side == 0 else EXT - HALO - 1 + d
        for group in range(groups):
            both = far_in[side, d - NEAR - 1, group].astype(f32)
            rows = pl.ds(8 * group, 8)
            fields[0][theirs, rows, pl.ds(0, half)] = both[:8]
            fields[0][theirs, rows, pl.ds(half, half)] = both[8:]

    def front(d):
        for side in range(2):
            @pl.when(has[side])
            def _():
                (near_wait if d <= NEAR else far_wait)(side, d)

        top, bottom = HALO - d, EXT - HALO - 1 + d
        for level in range(1, STEPS + 1):
            inside = d <= level
            row_step(level, top + level, None if inside else keeps[0], inside)
            row_step(level, bottom - level, None if inside else keeps[1], inside)

    for d in range(1, HALO + 1):
        front(d)

    values = [grams[i] for i in range(2 * STEPS)]

    def fold(low, high, shift, lanes):
        kept = low + pltpu.roll(low, LANES - shift, 1)
        if high is None:
            high = jnp.zeros_like(low)
        moved = high + pltpu.roll(high, shift, 1)
        return jnp.where((lanes & shift) == 0, kept, moved)

    shift = LANES // 2
    while len(values) > 1:
        middle = len(values) // 2
        values = [fold(values[i], values[i + middle], shift, lane) for i in range(middle)]
        shift //= 2
    values = [values[0][8 * g:8 * g + 8] for g in range(groups)] + [None] * (8 - groups)
    while len(values) > 1:
        middle = len(values) // 2
        values = [None if values[i] is None else fold(values[i], values[i + middle], shift, lane8)
                  for i in range(middle)]
        shift //= 2
    total = values[0]

    for phase, (stride, size) in enumerate(dims):
        place = places[phase]
        gather[phase, place] = total
        copies = []
        for step in range(1, size):
            there = tile + (lax.rem(place + step, size) - place) * stride
            copy = pltpu.make_async_remote_copy(
                src_ref=gather.at[phase, place], dst_ref=gather.at[phase, place],
                send_sem=red_send.at[phase, step - 1], recv_sem=red_recv.at[phase, step - 1],
                device_id={"tile": there}, device_id_type=MESH)
            copy.start()
            copies.append(copy)
        for copy in copies:
            copy.wait_recv()
        total = gather[phase, 0]
        for i in range(1, size):
            total = total + gather[phase, i]

    dots = [total if i == 0 else pltpu.roll(total, LANES - 8 * i, 1) for i in range(2 * STEPS)]
    moments = dots[:2]
    for i in range(2, 2 * STEPS):
        moments.append(dots[i] - dots[i - 2])
    zero = jnp.zeros_like(total)
    half_scale = 0.5 * scale
    r_mom, p_mom = list(moments), list(moments)
    r_co, p_co, x_co = [zero + 1.0], [zero + 1.0], []
    squares = moments[0]

    for step in range(STEPS):
        through = []
        for i in range(len(p_mom) - 1):
            around = p_mom[i + 1] if i == 0 else p_mom[i - 1] + p_mom[i + 1]
            through.append(p_mom[i] - half_scale * around)
        alpha = squares / add(p_co[i] * through[i] for i in range(step + 1))
        x_co = [x_co[i] + alpha * p_co[i] if i < len(x_co) else alpha * p_co[i] for i in range(step + 1)]
        grown = []
        for i in range(step + 2):
            terms = [p_co[k] for k in (i - 1, i + 1) if 0 <= k <= step]
            moved = p_co[i] if i <= step else zero
            if terms:
                moved = moved - half_scale * add(terms)
            grown.append(r_co[i] - alpha * moved if i < len(r_co) else -(alpha * moved))
        r_co = grown
        if step == STEPS - 1:
            break
        r_mom = [r_mom[i] - alpha * through[i] for i in range(len(through))]
        fresh = add(r_co[i] * r_mom[i] for i in range(step + 2))
        beta = fresh / squares
        squares = fresh
        p_co = [r_co[i] + beta * p_co[i] if i <= step else r_co[i] for i in range(step + 2)]
        p_mom = [r_mom[i] + beta * p_mom[i] for i in range(len(r_mom))]

    for i, value in enumerate(x_co + r_co):
        for group in range(groups):
            coef[i, pl.ds(8 * group, 8), :] = jnp.broadcast_to(value[:, group:group + 1], (8, LANES))

    for send in sends:
        send.wait_send()
    for side in range(2):
        @pl.when(has[side])
        def _():
            for d in range(1, NEAR + 1):
                for piece in range(2):
                    near_copy(side, d, piece).wait_send()
            for d in range(NEAR + 1, HALO + 1):
                far_copy(side, d).wait_send()
    for phase, (stride, size) in enumerate(dims):
        for step in range(1, size):
            pltpu.make_async_remote_copy(
                src_ref=gather.at[phase, places[phase]], dst_ref=gather.at[phase, places[phase]],
                send_sem=red_send.at[phase, step - 1], recv_sem=red_recv.at[phase, step - 1],
                device_id={"tile": tile}, device_id_type=MESH).wait_send()


def combine_kernel(*refs):
    coef, fields = refs[0], refs[1:STEPS + 2]
    sol_hbm, res_hbm, sol_rows, res_rows, out_sem = refs[STEPS + 2:]
    groups = fields[0].shape[1] // 8
    cols = fields[0].shape[2] // LANES

    def out_copy(which, row):
        source = (sol_rows, res_rows)[which].at[row]
        target = (sol_hbm, res_hbm)[which].at[:, row, :]
        return pltpu.make_async_copy(source, target, out_sem.at[which, row])

    def combine(pair, carry):
        def one_group(group, c):
            rows = pl.ds(pl.multiple_of(8 * group, 8), 8)
            factors = [coef[i, rows, :] for i in range(2 * STEPS + 1)]
            for more in range(2):
                row = 2 * pair + more
                for j in range(cols):
                    part = pl.ds(j * LANES, LANES)
                    parts = [fields[k][row + HALO - k, rows, part] for k in range(STEPS + 1)]
                    sol = add(factors[k] * parts[k] for k in range(STEPS))
                    res = add(factors[STEPS + k] * parts[k] for k in range(STEPS + 1))
                    sol_rows[row, rows, part] = sol
                    res_rows[row, rows, part] = res
            return c
        lax.fori_loop(0, groups, one_group, 0)
        for more in range(2):
            for which in range(2):
                out_copy(which, 2 * pair + more).start()
        return carry

    lax.fori_loop(0, ROWS // 2, combine, 0)

    def drain(row, carry):
        for which in range(2):
            out_copy(which, row).wait()
        return carry

    lax.fori_loop(0, ROWS, drain, 0)


def shards(dims, increments, projection, helmholtz):
    levels, rows, cells = increments.shape
    modes = projection.shape[0] // 2
    groups = modes // 8
    out = jax.ShapeDtypeStruct((modes, rows, cells), jnp.float32)
    longest = max(size for _, size in dims)
    hbm = pl.BlockSpec(memory_space=pltpu.HBM)
    dma = pltpu.SemaphoreType.DMA
    vmem = pl.BlockSpec(memory_space=pltpu.VMEM)
    kept = [pltpu.VMEM((2 * STEPS + 1, modes, LANES), jnp.float32)]
    kept += [pltpu.VMEM((EXT - 2 * k, modes, cells), jnp.float32) for k in range(STEPS + 1)]
    fields = pl.pallas_call(
        functools.partial(kernel, dims),
        out_shape=tuple(kept),
        in_specs=[hbm] * 3,
        out_specs=(vmem,) * len(kept),
        scratch_shapes=[
            pltpu.VMEM((levels, rows, cells), jnp.bfloat16),
            pltpu.VMEM((levels, rows, cells), jnp.bfloat16),
            pltpu.VMEM((2, rows * modes, rows * levels), jnp.bfloat16),
            pltpu.VMEM((2 * STEPS, modes, LANES), jnp.float32),
            pltpu.VMEM((2, HALO - NEAR, groups, 16, cells // 2), jnp.bfloat16),
            pltpu.VMEM((2, HALO - NEAR, groups, 16, cells // 2), jnp.bfloat16),
            pltpu.VMEM((len(dims), longest, 8, LANES), jnp.float32),
            dma((4,)), dma((4,)), dma((4,)),
            dma((2, NEAR, 2)), dma((2, NEAR, 2)),
            dma((2, HALO - NEAR)), dma((2, HALO - NEAR)),
            dma((len(dims), longest - 1)), dma((len(dims), longest - 1)),
            pltpu.VMEM((2 * levels, 2 * modes), jnp.bfloat16), pltpu.SMEM((modes,), jnp.float32), dma((2,)),
            pltpu.SemaphoreType.REGULAR((6,)),
        ],
        compiler_params=pltpu.CompilerParams(
            collective_id=0, has_side_effects=True, vmem_limit_bytes=14 * 1024 * 1024),
    )(*(pltpu.with_memory_space_constraint(x, pltpu.HBM) for x in (increments, projection.T, helmholtz)))
    return pl.pallas_call(
        combine_kernel,
        out_shape=(out, out),
        in_specs=[vmem] * len(kept),
        out_specs=(hbm, hbm),
        scratch_shapes=[
            pltpu.VMEM((rows, modes, cells), jnp.float32),
            pltpu.VMEM((rows, modes, cells), jnp.float32),
            dma((2, ROWS)),
        ],
        compiler_params=pltpu.CompilerParams(vmem_limit_bytes=10 * 1024 * 1024),
    )(*fields)


def solution(mesh):
    tiles = mesh.shape["tile"]
    dims = ((1, 4), (4, 4), (16, 4)) if tiles == 64 else ((1, 2), (2, 2), (4, 2))
    in_specs = (P("lev", "tile", None), P(), P("lev"))
    out_specs = (P("lev", "tile", None), P("lev", "tile", None))
    return jax.shard_map(functools.partial(shards, dims), mesh=mesh, in_specs=in_specs,
                         out_specs=out_specs, check_vma=False)
```

```python
import functools

import jax
import jax.numpy as jnp
from jax import lax
from jax.experimental import pallas as pl
from jax.experimental.pallas import tpu as pltpu
from jax.sharding import PartitionSpec as P

STEPS = 8
ROWS = 16
HALO = 8
EXT = ROWS + 2 * HALO
NEAR = 4
LANES = 128
MESH = pl.DeviceIdType.MESH


def add(items):
    items = list(items)
    while len(items) > 1:
        items = [items[i] + items[i + 1] if i + 1 < len(items) else items[i]
                 for i in range(0, len(items), 2)]
    return items[0]


def kernel(dims, inc_hbm, proj_hbm, helm_hbm, coef, *refs):
    fields = refs[:STEPS + 1]
    (inc_own, inc_far, kron, grams, far_out, far_in, gather,
     lev_send, lev_recv, load_sem, near_send, near_recv, far_send, far_recv,
     red_send, red_recv, proj_ref, helm_ref, small_sem, relay_sem) = refs[STEPS + 1:]
    tile = lax.axis_index("tile")
    lev = lax.axis_index("lev")
    tiles = lax.axis_size("tile")
    levels, _, cells = inc_own.shape
    modes = fields[0].shape[1]
    groups = modes // 8
    chunk = cells // 4
    cols = cells // LANES
    other = 1 - lev
    has = (tile > 0, tile < tiles - 1)
    partner = (tile - 1, tile + 1)
    f32 = jnp.float32

    barrier = pltpu.get_barrier_semaphore()
    pl.semaphore_signal(barrier, inc=1, device_id={"lev": other}, device_id_type=MESH)
    block = dims[2][0]
    corner = dims[1][0] * (dims[1][1] - 1)
    spot = lax.rem(tile, block)
    close = (spot != 0, spot != block - 1)
    for side in range(2):
        @pl.when(close[side])
        def _():
            pl.semaphore_signal(barrier, inc=1, device_id={"tile": partner[side]}, device_id_type=MESH)
    places = []
    for stride, size in dims:
        place = lax.rem(lax.div(tile, stride), size)
        places.append(place)
        for step in range(1, size):
            there = tile + (lax.rem(place + step, size) - place) * stride
            pl.semaphore_signal(barrier, inc=1, device_id={"tile": there}, device_id_type=MESH)

    loads = []
    for c in range(4):
        part = pl.ds(c * chunk, chunk)
        load = pltpu.make_async_copy(inc_hbm.at[:, :, part], inc_own.at[:, :, part], load_sem.at[c])
        load.start()
        loads.append(load)
    small = (pltpu.make_async_copy(proj_hbm, proj_ref, small_sem.at[0]),
             pltpu.make_async_copy(helm_hbm, helm_ref, small_sem.at[1]))
    for load in small:
        load.start()

    for side, base in ((0, 0), (1, EXT - HALO)):
        @pl.when(jnp.logical_not(has[side]))
        def _():
            def clear(row, carry):
                fields[0][row + base] = jnp.zeros((modes, cells), f32)
                return carry
            lax.fori_loop(0, HALO, clear, 0)
    wide = levels * ROWS
    for load in small:
        load.wait()
    table = proj_ref[...]
    at_row = lax.broadcasted_iota(jnp.int32, (modes, wide), 1) % ROWS
    of_level = (lax.broadcasted_iota(jnp.int32, (2 * levels, wide), 0)
                - lax.broadcasted_iota(jnp.int32, (2 * levels, wide), 1) // ROWS)
    for half in range(2):
        first_level = (lev if half == 0 else other) * levels
        spread = jnp.where(of_level == first_level, 1.0, 0.0).astype(jnp.bfloat16)
        repeated = lax.dot_general(table, spread, (((0,), (0,)), ((), ())), preferred_element_type=f32)
        repeated = jnp.where(lev == 0, repeated[:modes], repeated[modes:])
        for pair in range(ROWS // 2):
            both = jnp.concatenate([
                jnp.where(at_row == 2 * pair, repeated, 0.0),
                jnp.where(at_row == 2 * pair + 1, repeated, 0.0)], axis=0)
            kron[half, pl.ds(2 * modes * pair, 2 * modes), :] = both.astype(jnp.bfloat16)

    lane8 = lax.broadcasted_iota(jnp.int32, (8, LANES), 1)
    sub8 = lax.broadcasted_iota(jnp.int32, (8, LANES), 0)
    shifts = jnp.zeros((8, LANES), f32)
    for mode in range(modes):
        shifts = jnp.where((lane8 == mode // 8) & (sub8 == mode % 8), helm_ref[mode], shifts)
    scale = 4.0 / (4.0 + shifts)

    grams[...] = jnp.zeros_like(grams)

    peers = 1 + sum(size - 1 for _, size in dims)
    pl.semaphore_wait(barrier, peers + sum(jnp.where(close[side], 1, 0) for side in range(2)))

    sends = []
    for c in range(4):
        part = pl.ds(c * chunk, chunk)
        send = pltpu.make_async_remote_copy(
            src_ref=inc_hbm.at[:, :, part], dst_ref=inc_far.at[:, :, part],
            send_sem=lev_send.at[c], recv_sem=lev_recv.at[c],
            device_id={"lev": other}, device_id_type=MESH)
        send.start()
        sends.append(send)

    inner = tile + block < tiles
    ends = ((spot == block - 1) & inner, (spot == 0) & (tile > 0))
    relays = ((spot == corner) & inner, (spot == 0) & inner)

    def pass_on(condition, arrives, leaves, there):
        @pl.when(condition)
        def _():
            if arrives is not None:
                pl.semaphore_wait(relay_sem.at[arrives], 1)
            if leaves is not None:
                pl.semaphore_signal(relay_sem.at[leaves], inc=1, device_id={"tile": there}, device_id_type=MESH)

    pass_on(ends[1], None, 0, tile - block)
    pass_on(ends[0], None, 3, tile - (block - 1 - corner))

    for c in range(4):
        if c == 2:
            pass_on(relays[1], 0, 1, tile + corner)
            pass_on(relays[0], 3, 4, tile - corner)
        loads[c].wait()
        part = pl.ds(c * chunk, chunk)
        first = jnp.dot(kron[0], inc_own[:, :, part].reshape(wide, chunk), preferred_element_type=f32)
        fields[0][pl.ds(HALO, ROWS), :, part] = first.reshape(ROWS, modes, chunk)

    pass_on(relays[0], 1, 2, tile + (block - 1 - corner))
    pass_on(relays[1], 4, 5, tile + block)

    def near_copy(side, d, piece):
        mine = HALO + d - 1 if side == 0 else EXT - HALO - d
        theirs = EXT - HALO - 1 + d if side == 0 else HALO - d
        part = pl.ds(0, chunk) if piece == 0 else pl.ds(chunk, cells - chunk)
        return pltpu.make_async_remote_copy(
            src_ref=fields[0].at[mine, :, part], dst_ref=fields[0].at[theirs, :, part],
            send_sem=near_send.at[side, d - 1, piece], recv_sem=near_recv.at[1 - side, d - 1, piece],
            device_id={"tile": partner[side]}, device_id_type=MESH)

    def far_copy(side, d):
        return pltpu.make_async_remote_copy(
            src_ref=far_out.at[side, d - NEAR - 1], dst_ref=far_in.at[1 - side, d - NEAR - 1],
            send_sem=far_send.at[side, d - NEAR - 1], recv_sem=far_recv.at[1 - side, d - NEAR - 1],
            device_id={"tile": partner[side]}, device_id_type=MESH)

    for c in range(4):
        sends[c].wait_recv()
        part = pl.ds(c * chunk, chunk)
        second = jnp.dot(kron[1], inc_far[:, :, part].reshape(wide, chunk), preferred_element_type=f32)
        fields[0][pl.ds(HALO, ROWS), :, part] += second.reshape(ROWS, modes, chunk)
        if c == 0:
            pass_on(ends[0], 2, None, None)
            pass_on(ends[1], 5, None, None)
        if c in (0, 3):
            for d in range(1, NEAR + 1):
                for side in range(2):
                    @pl.when(has[side])
                    def _():
                        near_copy(side, d, 0 if c == 0 else 1).start()
    half = cells // 2
    for d in range(NEAR + 1, HALO + 1):
        for side in range(2):
            mine = HALO + d - 1 if side == 0 else EXT - HALO - d
            for group in range(groups):
                rows = pl.ds(8 * group, 8)
                both = jnp.concatenate(
                    [fields[0][mine, rows, pl.ds(0, half)], fields[0][mine, rows, pl.ds(half, half)]], axis=0)
                far_out[side, d - NEAR - 1, group] = both.astype(jnp.bfloat16)

            @pl.when(has[side])
            def _():
                far_copy(side, d).start()

    lane = lax.broadcasted_iota(jnp.int32, (modes, LANES), 1)
    at_first, at_last = lane == 0, lane == LANES - 1

    def row_step(level, row, keep=None, gram=True):
        source, new = fields[level - 1], fields[level]
        here, there = row - (level - 1), row - level
        turned = {}

        def turn(j):
            if j not in turned:
                value = source[here, :, pl.ds(j * LANES, LANES)]
                turned[j] = (value, pltpu.roll(value, 1, 1), pltpu.roll(value, LANES - 1, 1))
            return turned[j]

        squares = cross = None
        for j in range(cols):
            part = pl.ds(j * LANES, LANES)
            value, right_by, left_by = turn(j)
            before = turn(j - 1)[1] if j > 0 else 0.0
            after = turn(j + 1)[2] if j < cols - 1 else 0.0
            beside = (jnp.where(at_first, before, right_by) + jnp.where(at_last, after, left_by)
                      + (source[here - 1, :, part] + source[here + 1, :, part]))
            result = 0.5 * beside
            if level > 1:
                result = result - fields[level - 2][row - (level - 2), :, part]
            if keep is not None:
                result = result * keep
            new[there, :, part] = result
            if gram:
                squares = value * value if squares is None else squares + value * value
                cross = value * result if cross is None else cross + value * result
        if gram:
            grams[2 * level - 2] += squares
            grams[2 * level - 1] += cross

    for level in range(1, HALO):
        pairs = HALO - level

        def four(i, carry):
            for more in range(4):
                row_step(level, HALO + level + 4 * i + more)
            return carry

        lax.fori_loop(0, pairs // 2, four, 0)
        if pairs % 2:
            for more in range(2):
                row_step(level, HALO + level + 2 * pairs - 2 + more)

    keeps = tuple(jnp.where(has[side], 1.0, 0.0) for side in range(2))

    def near_wait(side, d):
        for piece in range(2):
            theirs = HALO - d if side == 0 else EXT - HALO - 1 + d
            part = pl.ds(0, chunk) if piece == 0 else pl.ds(chunk, cells - chunk)
            pltpu.make_async_remote_copy(
                src_ref=fields[0].at[theirs, :, part], dst_ref=fields[0].at[theirs, :, part],
                send_sem=near_send.at[side, d - 1, piece], recv_sem=near_recv.at[side, d - 1, piece],
                device_id={"tile": partner[side]}, device_id_type=MESH).wait_recv()

    def far_wait(side, d):
        pltpu.make_async_remote_copy(
            src_ref=far_in.at[side, d - NEAR - 1], dst_ref=far_in.at[side, d - NEAR - 1],
            send_sem=far_send.at[side, d - NEAR - 1], recv_sem=far_recv.at[side, d - NEAR - 1],
            device_id={"tile": partner[side]}, device_id_type=MESH).wait_recv()
        theirs = HALO - d if side == 0 else EXT - HALO - 1 + d
        for group in range(groups):
            both = far_in[side, d - NEAR - 1, group].astype(f32)
            rows = pl.ds(8 * group, 8)
            fields[0][theirs, rows, pl.ds(0, half)] = both[:8]
            fields[0][theirs, rows, pl.ds(half, half)] = both[8:]

    def front(d):
        for side in range(2):
            @pl.when(has[side])
            def _():
                (near_wait if d <= NEAR else far_wait)(side, d)

        top, bottom = HALO - d, EXT - HALO - 1 + d
        for level in range(1, STEPS + 1):
            inside = d <= level
            row_step(level, top + level, None if inside else keeps[0], inside)
            row_step(level, bottom - level, None if inside else keeps[1], inside)

    for d in range(1, HALO + 1):
        front(d)

    values = [grams[i] for i in range(2 * STEPS)]

    def fold(low, high, shift, lanes):
        kept = low + pltpu.roll(low, LANES - shift, 1)
        if high is None:
            high = jnp.zeros_like(low)
        moved = high + pltpu.roll(high, shift, 1)
        return jnp.where((lanes & shift) == 0, kept, moved)

    shift = LANES // 2
    while len(values) > 1:
        middle = len(values) // 2
        values = [fold(values[i], values[i + middle], shift, lane) for i in range(middle)]
        shift //= 2
    values = [values[0][8 * g:8 * g + 8] for g in range(groups)] + [None] * (8 - groups)
    while len(values) > 1:
        middle = len(values) // 2
        values = [None if values[i] is None else fold(values[i], values[i + middle], shift, lane8)
                  for i in range(middle)]
        shift //= 2
    total = values[0]

    for phase, (stride, size) in enumerate(dims):
        place = places[phase]
        gather[phase, place] = total
        copies = []
        for step in range(1, size):
            there = tile + (lax.rem(place + step, size) - place) * stride
            copy = pltpu.make_async_remote_copy(
                src_ref=gather.at[phase, place], dst_ref=gather.at[phase, place],
                send_sem=red_send.at[phase, step - 1], recv_sem=red_recv.at[phase, step - 1],
                device_id={"tile": there}, device_id_type=MESH)
            copy.start()
            copies.append(copy)
        for copy in copies:
            copy.wait_recv()
        total = gather[phase, 0]
        for i in range(1, size):
            total = total + gather[phase, i]

    dots = [total if i == 0 else pltpu.roll(total, LANES - 8 * i, 1) for i in range(2 * STEPS)]
    moments = dots[:2]
    for i in range(2, 2 * STEPS):
        moments.append(dots[i] - dots[i - 2])
    zero = jnp.zeros_like(total)
    half_scale = 0.5 * scale
    r_mom, p_mom = list(moments), list(moments)
    r_co, p_co, x_co = [zero + 1.0], [zero + 1.0], []
    squares = moments[0]

    for step in range(STEPS):
        through = []
        for i in range(len(p_mom) - 1):
            around = p_mom[i + 1] if i == 0 else p_mom[i - 1] + p_mom[i + 1]
            through.append(p_mom[i] - half_scale * around)
        alpha = squares / add(p_co[i] * through[i] for i in range(step + 1))
        x_co = [x_co[i] + alpha * p_co[i] if i < len(x_co) else alpha * p_co[i] for i in range(step + 1)]
        grown = []
        for i in range(step + 2):
            terms = [p_co[k] for k in (i - 1, i + 1) if 0 <= k <= step]
            moved = p_co[i] if i <= step else zero
            if terms:
                moved = moved - half_scale * add(terms)
            grown.append(r_co[i] - alpha * moved if i < len(r_co) else -(alpha * moved))
        r_co = grown
        if step == STEPS - 1:
            break
        r_mom = [r_mom[i] - alpha * through[i] for i in range(len(through))]
        fresh = add(r_co[i] * r_mom[i] for i in range(step + 2))
        beta = fresh / squares
        squares = fresh
        p_co = [r_co[i] + beta * p_co[i] if i <= step else r_co[i] for i in range(step + 2)]
        p_mom = [r_mom[i] + beta * p_mom[i] for i in range(len(r_mom))]

    for i, value in enumerate(x_co + r_co):
        for group in range(groups):
            coef[i, pl.ds(8 * group, 8), :] = jnp.broadcast_to(value[:, group:group + 1], (8, LANES))

    for send in sends:
        send.wait_send()
    for side in range(2):
        @pl.when(has[side])
        def _():
            for d in range(1, NEAR + 1):
                for piece in range(2):
                    near_copy(side, d, piece).wait_send()
            for d in range(NEAR + 1, HALO + 1):
                far_copy(side, d).wait_send()
    for phase, (stride, size) in enumerate(dims):
        for step in range(1, size):
            pltpu.make_async_remote_copy(
                src_ref=gather.at[phase, places[phase]], dst_ref=gather.at[phase, places[phase]],
                send_sem=red_send.at[phase, step - 1], recv_sem=red_recv.at[phase, step - 1],
                device_id={"tile": tile}, device_id_type=MESH).wait_send()


def combine_kernel(*refs):
    coef, fields = refs[0], refs[1:STEPS + 2]
    sol_hbm, res_hbm, sol_rows, res_rows, out_sem = refs[STEPS + 2:]
    groups = fields[0].shape[1] // 8
    cols = fields[0].shape[2] // LANES

    def out_copy(which, row):
        source = (sol_rows, res_rows)[which].at[row]
        target = (sol_hbm, res_hbm)[which].at[:, row, :]
        return pltpu.make_async_copy(source, target, out_sem.at[which, row])

    def combine(pair, carry):
        def one_group(group, c):
            rows = pl.ds(pl.multiple_of(8 * group, 8), 8)
            factors = [coef[i, rows, :] for i in range(2 * STEPS + 1)]
            for more in range(2):
                row = 2 * pair + more
                for j in range(cols):
                    part = pl.ds(j * LANES, LANES)
                    parts = [fields[k][row + HALO - k, rows, part] for k in range(STEPS + 1)]
                    sol = add(factors[k] * parts[k] for k in range(STEPS))
                    res = add(factors[STEPS + k] * parts[k] for k in range(STEPS + 1))
                    sol_rows[row, rows, part] = sol
                    res_rows[row, rows, part] = res
            return c
        lax.fori_loop(0, groups, one_group, 0)
        for more in range(2):
            for which in range(2):
                out_copy(which, 2 * pair + more).start()
        return carry

    lax.fori_loop(0, ROWS // 2, combine, 0)

    def drain(row, carry):
        for which in range(2):
            out_copy(which, row).wait()
        return carry

    lax.fori_loop(0, ROWS, drain, 0)


def shards(dims, increments, projection, helmholtz):
    levels, rows, cells = increments.shape
    modes = projection.shape[0] // 2
    groups = modes // 8
    out = jax.ShapeDtypeStruct((modes, rows, cells), jnp.float32)
    longest = max(size for _, size in dims)
    hbm = pl.BlockSpec(memory_space=pltpu.HBM)
    dma = pltpu.SemaphoreType.DMA
    vmem = pl.BlockSpec(memory_space=pltpu.VMEM)
    kept = [pltpu.VMEM((2 * STEPS + 1, modes, LANES), jnp.float32)]
    kept += [pltpu.VMEM((EXT - 2 * k, modes, cells), jnp.float32) for k in range(STEPS + 1)]
    fields = pl.pallas_call(
        functools.partial(kernel, dims),
        out_shape=tuple(kept),
        in_specs=[hbm] * 3,
        out_specs=(vmem,) * len(kept),
        scratch_shapes=[
            pltpu.VMEM((levels, rows, cells), jnp.bfloat16),
            pltpu.VMEM((levels, rows, cells), jnp.bfloat16),
            pltpu.VMEM((2, rows * modes, rows * levels), jnp.bfloat16),
            pltpu.VMEM((2 * STEPS, modes, LANES), jnp.float32),
            pltpu.VMEM((2, HALO - NEAR, groups, 16, cells // 2), jnp.bfloat16),
            pltpu.VMEM((2, HALO - NEAR, groups, 16, cells // 2), jnp.bfloat16),
            pltpu.VMEM((len(dims), longest, 8, LANES), jnp.float32),
            dma((4,)), dma((4,)), dma((4,)),
            dma((2, NEAR, 2)), dma((2, NEAR, 2)),
            dma((2, HALO - NEAR)), dma((2, HALO - NEAR)),
            dma((len(dims), longest - 1)), dma((len(dims), longest - 1)),
            pltpu.VMEM((2 * levels, 2 * modes), jnp.bfloat16), pltpu.SMEM((modes,), jnp.float32), dma((2,)),
            pltpu.SemaphoreType.REGULAR((6,)),
        ],
        compiler_params=pltpu.CompilerParams(
            collective_id=0, has_side_effects=True, vmem_limit_bytes=14 * 1024 * 1024),
    )(*(pltpu.with_memory_space_constraint(x, pltpu.HBM) for x in (increments, projection.T, helmholtz)))
    return pl.pallas_call(
        combine_kernel,
        out_shape=(out, out),
        in_specs=[vmem] * len(kept),
        out_specs=(hbm, hbm),
        scratch_shapes=[
            pltpu.VMEM((rows, modes, cells), jnp.float32),
            pltpu.VMEM((rows, modes, cells), jnp.float32),
            dma((2, ROWS)),
        ],
        compiler_params=pltpu.CompilerParams(vmem_limit_bytes=10 * 1024 * 1024),
    )(*fields)


def solution(mesh):
    tiles = mesh.shape["tile"]
    dims = ((1, 4), (4, 4), (16, 4)) if tiles == 64 else ((1, 2), (2, 2), (4, 2))
    in_specs = (P("lev", "tile", None), P(), P("lev"))
    out_specs = (P("lev", "tile", None), P("lev", "tile", None))
    return jax.shard_map(functools.partial(shards, dims), mesh=mesh, in_specs=in_specs,
                         out_specs=out_specs, check_vma=False)
```

```python
import functools

import jax
import jax.numpy as jnp
from jax import lax
from jax.experimental import pallas as pl
from jax.experimental.pallas import tpu as pltpu
from jax.sharding import PartitionSpec as P

STEPS = 8
ROWS = 16
HALO = 8
EXT = ROWS + 2 * HALO
NEAR = 4
LANES = 128
MESH = pl.DeviceIdType.MESH


def add(items):
    items = list(items)
    while len(items) > 1:
        items = [items[i] + items[i + 1] if i + 1 < len(items) else items[i]
                 for i in range(0, len(items), 2)]
    return items[0]


def kernel(dims, inc_hbm, proj_hbm, helm_hbm, coef, *refs):
    fields = refs[:STEPS + 1]
    (inc_own, inc_far, kron, grams, far_out, far_in, gather,
     lev_send, lev_recv, load_sem, near_send, near_recv, far_send, far_recv,
     red_send, red_recv, proj_ref, helm_ref, small_sem, relay_sem) = refs[STEPS + 1:]
    tile = lax.axis_index("tile")
    lev = lax.axis_index("lev")
    tiles = lax.axis_size("tile")
    levels, _, cells = inc_own.shape
    modes = fields[0].shape[1]
    groups = modes // 8
    chunk = cells // 4
    cols = cells // LANES
    other = 1 - lev
    has = (tile > 0, tile < tiles - 1)
    partner = (tile - 1, tile + 1)
    f32 = jnp.float32

    barrier = pltpu.get_barrier_semaphore()
    pl.semaphore_signal(barrier, inc=1, device_id={"lev": other}, device_id_type=MESH)
    block = dims[2][0]
    corner = dims[1][0] * (dims[1][1] - 1)
    spot = lax.rem(tile, block)
    close = (spot != 0, spot != block - 1)
    for side in range(2):
        @pl.when(close[side])
        def _():
            pl.semaphore_signal(barrier, inc=1, device_id={"tile": partner[side]}, device_id_type=MESH)
    places = []
    for stride, size in dims:
        place = lax.rem(lax.div(tile, stride), size)
        places.append(place)
        for step in range(1, size):
            there = tile + (lax.rem(place + step, size) - place) * stride
            pl.semaphore_signal(barrier, inc=1, device_id={"tile": there}, device_id_type=MESH)

    loads = []
    for c in range(4):
        part = pl.ds(c * chunk, chunk)
        load = pltpu.make_async_copy(inc_hbm.at[:, :, part], inc_own.at[:, :, part], load_sem.at[c])
        load.start()
        loads.append(load)
    small = (pltpu.make_async_copy(proj_hbm, proj_ref, small_sem.at[0]),
             pltpu.make_async_copy(helm_hbm, helm_ref, small_sem.at[1]))
    for load in small:
        load.start()

    for side, base in ((0, 0), (1, EXT - HALO)):
        @pl.when(jnp.logical_not(has[side]))
        def _():
            def clear(row, carry):
                fields[0][row + base] = jnp.zeros((modes, cells), f32)
                return carry
            lax.fori_loop(0, HALO, clear, 0)
    wide = levels * ROWS
    for load in small:
        load.wait()
    table = proj_ref[...]
    at_row = lax.broadcasted_iota(jnp.int32, (modes, wide), 1) % ROWS
    of_level = (lax.broadcasted_iota(jnp.int32, (2 * levels, wide), 0)
                - lax.broadcasted_iota(jnp.int32, (2 * levels, wide), 1) // ROWS)
    for half in range(2):
        first_level = (lev if half == 0 else other) * levels
        spread = jnp.where(of_level == first_level, 1.0, 0.0).astype(jnp.bfloat16)
        repeated = lax.dot_general(table, spread, (((0,), (0,)), ((), ())), preferred_element_type=f32)
        repeated = jnp.where(lev == 0, repeated[:modes], repeated[modes:])
        for pair in range(ROWS // 2):
            both = jnp.concatenate([
                jnp.where(at_row == 2 * pair, repeated, 0.0),
                jnp.where(at_row == 2 * pair + 1, repeated, 0.0)], axis=0)
            kron[half, pl.ds(2 * modes * pair, 2 * modes), :] = both.astype(jnp.bfloat16)

    lane8 = lax.broadcasted_iota(jnp.int32, (8, LANES), 1)
    sub8 = lax.broadcasted_iota(jnp.int32, (8, LANES), 0)
    shifts = jnp.zeros((8, LANES), f32)
    for mode in range(modes):
        shifts = jnp.where((lane8 == mode // 8) & (sub8 == mode % 8), helm_ref[mode], shifts)
    scale = 4.0 / (4.0 + shifts)

    grams[...] = jnp.zeros_like(grams)

    peers = 1 + sum(size - 1 for _, size in dims)
    pl.semaphore_wait(barrier, peers + sum(jnp.where(close[side], 1, 0) for side in range(2)))

    sends = []
    for c in range(4):
        part = pl.ds(c * chunk, chunk)
        send = pltpu.make_async_remote_copy(
            src_ref=inc_hbm.at[:, :, part], dst_ref=inc_far.at[:, :, part],
            send_sem=lev_send.at[c], recv_sem=lev_recv.at[c],
            device_id={"lev": other}, device_id_type=MESH)
        send.start()
        sends.append(send)

    inner = tile + block < tiles
    ends = ((spot == block - 1) & inner, (spot == 0) & (tile > 0))
    relays = ((spot == corner) & inner, (spot == 0) & inner)

    def pass_on(condition, arrives, leaves, there):
        @pl.when(condition)
        def _():
            if arrives is not None:
                pl.semaphore_wait(relay_sem.at[arrives], 1)
            if leaves is not None:
                pl.semaphore_signal(relay_sem.at[leaves], inc=1, device_id={"tile": there}, device_id_type=MESH)

    pass_on(ends[1], None, 0, tile - block)
    pass_on(ends[0], None, 3, tile - (block - 1 - corner))

    for c in range(4):
        if c == 2:
            pass_on(relays[1], 0, 1, tile + corner)
            pass_on(relays[0], 3, 4, tile - corner)
        loads[c].wait()
        part = pl.ds(c * chunk, chunk)
        first = jnp.dot(kron[0], inc_own[:, :, part].reshape(wide, chunk), preferred_element_type=f32)
        fields[0][pl.ds(HALO, ROWS), :, part] = first.reshape(ROWS, modes, chunk)

    pass_on(relays[0], 1, 2, tile + (block - 1 - corner))
    pass_on(relays[1], 4, 5, tile + block)

    def near_copy(side, d, piece):
        mine = HALO + d - 1 if side == 0 else EXT - HALO - d
        theirs = EXT - HALO - 1 + d if side == 0 else HALO - d
        part = pl.ds(0, chunk) if piece == 0 else pl.ds(chunk, cells - chunk)
        return pltpu.make_async_remote_copy(
            src_ref=fields[0].at[mine, :, part], dst_ref=fields[0].at[theirs, :, part],
            send_sem=near_send.at[side, d - 1, piece], recv_sem=near_recv.at[1 - side, d - 1, piece],
            device_id={"tile": partner[side]}, device_id_type=MESH)

    def far_copy(side, d):
        return pltpu.make_async_remote_copy(
            src_ref=far_out.at[side, d - NEAR - 1], dst_ref=far_in.at[1 - side, d - NEAR - 1],
            send_sem=far_send.at[side, d - NEAR - 1], recv_sem=far_recv.at[1 - side, d - NEAR - 1],
            device_id={"tile": partner[side]}, device_id_type=MESH)

    for c in range(4):
        sends[c].wait_recv()
        part = pl.ds(c * chunk, chunk)
        second = jnp.dot(kron[1], inc_far[:, :, part].reshape(wide, chunk), preferred_element_type=f32)
        fields[0][pl.ds(HALO, ROWS), :, part] += second.reshape(ROWS, modes, chunk)
        if c == 0:
            pass_on(ends[0], 2, None, None)
            pass_on(ends[1], 5, None, None)
        if c in (0, 3):
            for d in range(1, NEAR + 1):
                for side in range(2):
                    @pl.when(has[side])
                    def _():
                        near_copy(side, d, 0 if c == 0 else 1).start()
    half = cells // 2
    for d in range(NEAR + 1, HALO + 1):
        for side in range(2):
            mine = HALO + d - 1 if side == 0 else EXT - HALO - d
            for group in range(groups):
                rows = pl.ds(8 * group, 8)
                both = jnp.concatenate(
                    [fields[0][mine, rows, pl.ds(0, half)], fields[0][mine, rows, pl.ds(half, half)]], axis=0)
                far_out[side, d - NEAR - 1, group] = both.astype(jnp.bfloat16)

            @pl.when(has[side])
            def _():
                far_copy(side, d).start()

    lane = lax.broadcasted_iota(jnp.int32, (modes, LANES), 1)
    at_first, at_last = lane == 0, lane == LANES - 1

    def row_step(level, row, keep=None, gram=True, stage="all", outward=0):
        source, new = fields[level - 1], fields[level]
        here, there = row - (level - 1), row - level
        turned = {}

        def turn(j):
            if j not in turned:
                value = source[here, :, pl.ds(j * LANES, LANES)]
                turned[j] = (value, pltpu.roll(value, 1, 1), pltpu.roll(value, LANES - 1, 1))
            return turned[j]

        squares = cross = None
        for j in range(cols):
            part = pl.ds(j * LANES, LANES)
            if stage == "finish":
                value = source[here, :, part]
                result = new[there, :, part] + 0.5 * source[here + outward, :, part]
            else:
                value, right_by, left_by = turn(j)
                before = turn(j - 1)[1] if j > 0 else 0.0
                after = turn(j + 1)[2] if j < cols - 1 else 0.0
                beside = jnp.where(at_first, before, right_by) + jnp.where(at_last, after, left_by)
                if stage == "all":
                    beside = beside + (source[here - 1, :, part] + source[here + 1, :, part])
                else:
                    beside = beside + source[here - outward, :, part]
                result = 0.5 * beside
                if level > 1:
                    result = result - fields[level - 2][row - (level - 2), :, part]
            if keep is not None and stage != "ahead":
                result = result * keep
            new[there, :, part] = result
            if gram and stage != "ahead":
                squares = value * value if squares is None else squares + value * value
                cross = value * result if cross is None else cross + value * result
        if gram and stage != "ahead":
            grams[2 * level - 2] += squares
            grams[2 * level - 1] += cross

    for level in range(1, HALO):
        pairs = HALO - level

        def four(i, carry):
            for more in range(4):
                row_step(level, HALO + level + 4 * i + more)
            return carry

        lax.fori_loop(0, pairs // 2, four, 0)
        if pairs % 2:
            for more in range(2):
                row_step(level, HALO + level + 2 * pairs - 2 + more)

    keeps = tuple(jnp.where(has[side], 1.0, 0.0) for side in range(2))

    def near_wait(side, d):
        for piece in range(2):
            theirs = HALO - d if side == 0 else EXT - HALO - 1 + d
            part = pl.ds(0, chunk) if piece == 0 else pl.ds(chunk, cells - chunk)
            pltpu.make_async_remote_copy(
                src_ref=fields[0].at[theirs, :, part], dst_ref=fields[0].at[theirs, :, part],
                send_sem=near_send.at[side, d - 1, piece], recv_sem=near_recv.at[side, d - 1, piece],
                device_id={"tile": partner[side]}, device_id_type=MESH).wait_recv()

    def far_wait(side, d):
        pltpu.make_async_remote_copy(
            src_ref=far_in.at[side, d - NEAR - 1], dst_ref=far_in.at[side, d - NEAR - 1],
            send_sem=far_send.at[side, d - NEAR - 1], recv_sem=far_recv.at[side, d - NEAR - 1],
            device_id={"tile": partner[side]}, device_id_type=MESH).wait_recv()
        theirs = HALO - d if side == 0 else EXT - HALO - 1 + d
        for group in range(groups):
            both = far_in[side, d - NEAR - 1, group].astype(f32)
            rows = pl.ds(8 * group, 8)
            fields[0][theirs, rows, pl.ds(0, half)] = both[:8]
            fields[0][theirs, rows, pl.ds(half, half)] = both[8:]

    def front(d):
        top, bottom = HALO - d, EXT - HALO - 1 + d
        last = d == HALO
        if last:
            for level in range(1, STEPS + 1):
                row_step(level, top + level, stage="ahead", outward=-1)
                row_step(level, bottom - level, stage="ahead", outward=1)
        for side in range(2):
            @pl.when(has[side])
            def _():
                (near_wait if d <= NEAR else far_wait)(side, d)
        for level in range(1, STEPS + 1):
            inside = d <= level
            stage = "finish" if last else "all"
            row_step(level, top + level, None if inside else keeps[0], inside, stage, -1)
            row_step(level, bottom - level, None if inside else keeps[1], inside, stage, 1)

    for d in range(1, HALO + 1):
        front(d)

    values = [grams[i] for i in range(2 * STEPS)]

    def fold(low, high, shift, lanes):
        kept = low + pltpu.roll(low, LANES - shift, 1)
        if high is None:
            high = jnp.zeros_like(low)
        moved = high + pltpu.roll(high, shift, 1)
        return jnp.where((lanes & shift) == 0, kept, moved)

    shift = LANES // 2
    while len(values) > 1:
        middle = len(values) // 2
        values = [fold(values[i], values[i + middle], shift, lane) for i in range(middle)]
        shift //= 2
    values = [values[0][8 * g:8 * g + 8] for g in range(groups)] + [None] * (8 - groups)
    while len(values) > 1:
        middle = len(values) // 2
        values = [None if values[i] is None else fold(values[i], values[i + middle], shift, lane8)
                  for i in range(middle)]
        shift //= 2
    total = values[0]

    for phase, (stride, size) in enumerate(dims):
        place = places[phase]
        gather[phase, place] = total
        copies = []
        for step in range(1, size):
            there = tile + (lax.rem(place + step, size) - place) * stride
            copy = pltpu.make_async_remote_copy(
                src_ref=gather.at[phase, place], dst_ref=gather.at[phase, place],
                send_sem=red_send.at[phase, step - 1], recv_sem=red_recv.at[phase, step - 1],
                device_id={"tile": there}, device_id_type=MESH)
            copy.start()
            copies.append(copy)
        for copy in copies:
            copy.wait_recv()
        total = gather[phase, 0]
        for i in range(1, size):
            total = total + gather[phase, i]

    dots = [total if i == 0 else pltpu.roll(total, LANES - 8 * i, 1) for i in range(2 * STEPS)]
    moments = dots[:2]
    for i in range(2, 2 * STEPS):
        moments.append(dots[i] - dots[i - 2])
    zero = jnp.zeros_like(total)
    half_scale = 0.5 * scale
    r_mom, p_mom = list(moments), list(moments)
    r_co, p_co, x_co = [zero + 1.0], [zero + 1.0], []
    squares = moments[0]

    for step in range(STEPS):
        through = []
        for i in range(len(p_mom) - 1):
            around = p_mom[i + 1] if i == 0 else p_mom[i - 1] + p_mom[i + 1]
            through.append(p_mom[i] - half_scale * around)
        alpha = squares / add(p_co[i] * through[i] for i in range(step + 1))
        x_co = [x_co[i] + alpha * p_co[i] if i < len(x_co) else alpha * p_co[i] for i in range(step + 1)]
        grown = []
        for i in range(step + 2):
            terms = [p_co[k] for k in (i - 1, i + 1) if 0 <= k <= step]
            moved = p_co[i] if i <= step else zero
            if terms:
                moved = moved - half_scale * add(terms)
            grown.append(r_co[i] - alpha * moved if i < len(r_co) else -(alpha * moved))
        r_co = grown
        if step == STEPS - 1:
            break
        r_mom = [r_mom[i] - alpha * through[i] for i in range(len(through))]
        fresh = add(r_co[i] * r_mom[i] for i in range(step + 2))
        beta = fresh / squares
        squares = fresh
        p_co = [r_co[i] + beta * p_co[i] if i <= step else r_co[i] for i in range(step + 2)]
        p_mom = [r_mom[i] + beta * p_mom[i] for i in range(len(r_mom))]

    for i, value in enumerate(x_co + r_co):
        for group in range(groups):
            coef[i, pl.ds(8 * group, 8), :] = jnp.broadcast_to(value[:, group:group + 1], (8, LANES))

    for send in sends:
        send.wait_send()
    for side in range(2):
        @pl.when(has[side])
        def _():
            for d in range(1, NEAR + 1):
                for piece in range(2):
                    near_copy(side, d, piece).wait_send()
            for d in range(NEAR + 1, HALO + 1):
                far_copy(side, d).wait_send()
    for phase, (stride, size) in enumerate(dims):
        for step in range(1, size):
            pltpu.make_async_remote_copy(
                src_ref=gather.at[phase, places[phase]], dst_ref=gather.at[phase, places[phase]],
                send_sem=red_send.at[phase, step - 1], recv_sem=red_recv.at[phase, step - 1],
                device_id={"tile": tile}, device_id_type=MESH).wait_send()


def combine_kernel(*refs):
    coef, fields = refs[0], refs[1:STEPS + 2]
    sol_hbm, res_hbm, sol_rows, res_rows, out_sem = refs[STEPS + 2:]
    groups = fields[0].shape[1] // 8
    cols = fields[0].shape[2] // LANES

    def out_copy(which, row):
        source = (sol_rows, res_rows)[which].at[row]
        target = (sol_hbm, res_hbm)[which].at[:, row, :]
        return pltpu.make_async_copy(source, target, out_sem.at[which, row])

    def combine(pair, carry):
        def one_group(group, c):
            rows = pl.ds(pl.multiple_of(8 * group, 8), 8)
            factors = [coef[i, rows, :] for i in range(2 * STEPS + 1)]
            for more in range(2):
                row = 2 * pair + more
                for j in range(cols):
                    part = pl.ds(j * LANES, LANES)
                    parts = [fields[k][row + HALO - k, rows, part] for k in range(STEPS + 1)]
                    sol = add(factors[k] * parts[k] for k in range(STEPS))
                    res = add(factors[STEPS + k] * parts[k] for k in range(STEPS + 1))
                    sol_rows[row, rows, part] = sol
                    res_rows[row, rows, part] = res
            return c
        lax.fori_loop(0, groups, one_group, 0)
        for more in range(2):
            for which in range(2):
                out_copy(which, 2 * pair + more).start()
        return carry

    lax.fori_loop(0, ROWS // 2, combine, 0)

    def drain(row, carry):
        for which in range(2):
            out_copy(which, row).wait()
        return carry

    lax.fori_loop(0, ROWS, drain, 0)


def shards(dims, increments, projection, helmholtz):
    levels, rows, cells = increments.shape
    modes = projection.shape[0] // 2
    groups = modes // 8
    out = jax.ShapeDtypeStruct((modes, rows, cells), jnp.float32)
    longest = max(size for _, size in dims)
    hbm = pl.BlockSpec(memory_space=pltpu.HBM)
    dma = pltpu.SemaphoreType.DMA
    vmem = pl.BlockSpec(memory_space=pltpu.VMEM)
    kept = [pltpu.VMEM((2 * STEPS + 1, modes, LANES), jnp.float32)]
    kept += [pltpu.VMEM((EXT - 2 * k, modes, cells), jnp.float32) for k in range(STEPS + 1)]
    fields = pl.pallas_call(
        functools.partial(kernel, dims),
        out_shape=tuple(kept),
        in_specs=[hbm] * 3,
        out_specs=(vmem,) * len(kept),
        scratch_shapes=[
            pltpu.VMEM((levels, rows, cells), jnp.bfloat16),
            pltpu.VMEM((levels, rows, cells), jnp.bfloat16),
            pltpu.VMEM((2, rows * modes, rows * levels), jnp.bfloat16),
            pltpu.VMEM((2 * STEPS, modes, LANES), jnp.float32),
            pltpu.VMEM((2, HALO - NEAR, groups, 16, cells // 2), jnp.bfloat16),
            pltpu.VMEM((2, HALO - NEAR, groups, 16, cells // 2), jnp.bfloat16),
            pltpu.VMEM((len(dims), longest, 8, LANES), jnp.float32),
            dma((4,)), dma((4,)), dma((4,)),
            dma((2, NEAR, 2)), dma((2, NEAR, 2)),
            dma((2, HALO - NEAR)), dma((2, HALO - NEAR)),
            dma((len(dims), longest - 1)), dma((len(dims), longest - 1)),
            pltpu.VMEM((2 * levels, 2 * modes), jnp.bfloat16), pltpu.SMEM((modes,), jnp.float32), dma((2,)),
            pltpu.SemaphoreType.REGULAR((6,)),
        ],
        compiler_params=pltpu.CompilerParams(
            collective_id=0, has_side_effects=True, vmem_limit_bytes=14 * 1024 * 1024),
    )(*(pltpu.with_memory_space_constraint(x, pltpu.HBM) for x in (increments, projection.T, helmholtz)))
    return pl.pallas_call(
        combine_kernel,
        out_shape=(out, out),
        in_specs=[vmem] * len(kept),
        out_specs=(hbm, hbm),
        scratch_shapes=[
            pltpu.VMEM((rows, modes, cells), jnp.float32),
            pltpu.VMEM((rows, modes, cells), jnp.float32),
            dma((2, ROWS)),
        ],
        compiler_params=pltpu.CompilerParams(vmem_limit_bytes=10 * 1024 * 1024),
    )(*fields)


def solution(mesh):
    tiles = mesh.shape["tile"]
    dims = ((1, 4), (4, 4), (16, 4)) if tiles == 64 else ((1, 2), (2, 2), (4, 2))
    in_specs = (P("lev", "tile", None), P(), P("lev"))
    out_specs = (P("lev", "tile", None), P("lev", "tile", None))
    return jax.shard_map(functools.partial(shards, dims), mesh=mesh, in_specs=in_specs,
                         out_specs=out_specs, check_vma=False)
```
